128 devices in a mesh: pod: 1, data: 64 (over z, y, x), model: 2 (over core).
Axes of the slice: x: 4, y: 4, z: 4, core: 2. Of those that a mesh axis runs over, the one named last changes fastest.
Arguments:
- x_in: bfloat16 [64, 1024, 2048], P(('pod', 'data'), 'model')
- dy_in: bfloat16 [64, 1024, 2048], P(('pod', 'data'), 'model')
- w_q: bfloat16 [2048, 8, 256], P(None, 'model')
- w_k: bfloat16 [1, 2048, 256], replicated
- w_v: bfloat16 [1, 2048, 256], replicated
- w_o: bfloat16 [8, 256, 2048], P('model')
Outputs:
- output 1: bfloat16 [64, 1024, 2048], P(('pod', 'data'), 'model')
- output 2: float32 [2048, 8, 256], P(('pod', 'data'), 'model')
- output 3: float32 [2048, 256], P(('pod', 'model', 'data'))
- output 4: float32 [2048, 256], P(('pod', 'model', 'data'))
- output 5: float32 [8, 256, 2048], P(('pod', 'model'), None, 'data')
All inputs are finite; a program needn't handle non-finite values.
Results may differ from the reference program's by a relative error of at most 0.0103.
Values are sent between devices in bfloat16 or wider.
A program may use at most 1 GiB of HBM per device.

```python
import jax
import jax.numpy as jnp
from jax import lax

NUM_SEQS = 64
SEQ_LEN = 1024
MODEL_DIM = 2048
Q_HEADS = 8
KV_HEADS = 1
HEAD_DIM = 256

GROUP_HEADS = Q_HEADS // KV_HEADS


def setup_inputs(seed: int = 0, part: int = 0) -> dict:
    shared_key = jax.random.key(seed)
    part_key = jax.random.fold_in(jax.random.key(seed + 1), part)
    key_x, key_dy = jax.random.split(part_key, 2)
    key_wq, key_wk, key_wv, key_wo = jax.random.split(shared_key, 4)
    act_shape = (NUM_SEQS, SEQ_LEN, MODEL_DIM)
    in_scale = MODEL_DIM ** -0.5
    out_scale = (Q_HEADS * HEAD_DIM) ** -0.5
    x_in = jax.random.normal(key_x, act_shape, jnp.float32)
    dy_in = jax.random.normal(key_dy, act_shape, jnp.float32)
    w_q = jax.random.normal(key_wq, (MODEL_DIM, Q_HEADS, HEAD_DIM), jnp.float32) * in_scale
    w_k = jax.random.normal(key_wk, (KV_HEADS, MODEL_DIM, HEAD_DIM), jnp.float32) * in_scale
    w_v = jax.random.normal(key_wv, (KV_HEADS, MODEL_DIM, HEAD_DIM), jnp.float32) * in_scale
    w_o = jax.random.normal(key_wo, (Q_HEADS, HEAD_DIM, MODEL_DIM), jnp.float32) * out_scale
    return {'x_in': x_in.astype(jnp.bfloat16), 'dy_in': dy_in.astype(jnp.bfloat16),
            'w_q': w_q.astype(jnp.bfloat16), 'w_k': w_k.astype(jnp.bfloat16),
            'w_v': w_v.astype(jnp.bfloat16), 'w_o': w_o.astype(jnp.bfloat16)}


def group_attention(operands):
    q_grp, k_one, v_one, dout_grp = operands
    score_scale = HEAD_DIM ** -0.5
    q_f32 = q_grp.astype(jnp.float32)
    k_f32 = k_one.astype(jnp.float32)
    v_f32 = v_one.astype(jnp.float32)
    dout_f32 = dout_grp.astype(jnp.float32)
    positions = jnp.arange(SEQ_LEN)
    causal = positions[:, None] >= positions[None, :]
    scores = jnp.einsum('qhe,ke->hqk', q_f32, k_f32) * score_scale
    attn_prob = jax.nn.softmax(jnp.where(causal, scores, -jnp.inf), axis=-1)
    prob_bf = attn_prob.astype(jnp.bfloat16).astype(jnp.float32)
    attn_out = jnp.einsum('hqk,ke->qhe', prob_bf, v_f32).astype(jnp.bfloat16)
    grad_prob = jnp.einsum('qhe,ke->hqk', dout_f32, v_f32)
    row_delta = jnp.einsum('qhe,qhe->hq', dout_f32, attn_out.astype(jnp.float32))
    grad_score = (attn_prob * (grad_prob - row_delta[:, :, None])).astype(jnp.bfloat16).astype(jnp.float32)
    grad_q = (jnp.einsum('hqk,ke->qhe', grad_score, k_f32) * score_scale).astype(jnp.bfloat16)
    grad_k = (jnp.einsum('hqk,qhe->ke', grad_score, q_f32) * score_scale).astype(jnp.bfloat16)
    grad_v = jnp.einsum('hqk,qhe->ke', prob_bf, dout_f32).astype(jnp.bfloat16)
    return attn_out, grad_q, grad_k, grad_v


def heads_to_items(per_head):
    return per_head.reshape(NUM_SEQS, SEQ_LEN, KV_HEADS, GROUP_HEADS, HEAD_DIM).transpose(0, 2, 1, 3, 4).reshape(NUM_SEQS * KV_HEADS, SEQ_LEN, GROUP_HEADS, HEAD_DIM)


def items_to_heads(per_item):
    return per_item.reshape(NUM_SEQS, KV_HEADS, SEQ_LEN, GROUP_HEADS, HEAD_DIM).transpose(0, 2, 1, 3, 4).reshape(NUM_SEQS, SEQ_LEN, Q_HEADS, HEAD_DIM)


def reference(x_in, dy_in, w_q, w_k, w_v, w_o):
    x_f32 = x_in.astype(jnp.float32)
    dy_f32 = dy_in.astype(jnp.float32)
    wq_f32 = w_q.astype(jnp.float32)
    wk_f32 = w_k.astype(jnp.float32)
    wv_f32 = w_v.astype(jnp.float32)
    wo_f32 = w_o.astype(jnp.float32)
    q_proj = jnp.einsum('std,dhe->sthe', x_f32, wq_f32).astype(jnp.bfloat16)
    k_proj = jnp.einsum('std,jde->sjte', x_f32, wk_f32).astype(jnp.bfloat16)
    v_proj = jnp.einsum('std,jde->sjte', x_f32, wv_f32).astype(jnp.bfloat16)
    dout_proj = jnp.einsum('std,hed->sthe', dy_f32, wo_f32).astype(jnp.bfloat16)
    item_count = NUM_SEQS * KV_HEADS
    attn_out, grad_q, grad_k, grad_v = lax.map(group_attention, (
        heads_to_items(q_proj), k_proj.reshape(item_count, SEQ_LEN, HEAD_DIM),
        v_proj.reshape(item_count, SEQ_LEN, HEAD_DIM), heads_to_items(dout_proj)))
    out_f32 = items_to_heads(attn_out).astype(jnp.float32)
    gq_f32 = items_to_heads(grad_q).astype(jnp.float32)
    gk_f32 = grad_k.reshape(NUM_SEQS, KV_HEADS, SEQ_LEN, HEAD_DIM).astype(jnp.float32)
    gv_f32 = grad_v.reshape(NUM_SEQS, KV_HEADS, SEQ_LEN, HEAD_DIM).astype(jnp.float32)
    dw_q = jnp.einsum('std,sthe->dhe', x_f32, gq_f32)
    dw_k = jnp.einsum('std,sjte->jde', x_f32, gk_f32).reshape(KV_HEADS * MODEL_DIM, HEAD_DIM)
    dw_v = jnp.einsum('std,sjte->jde', x_f32, gv_f32).reshape(KV_HEADS * MODEL_DIM, HEAD_DIM)
    dw_o = jnp.einsum('sthe,std->hed', out_f32, dy_f32)
    dx_f32 = (jnp.einsum('sthe,dhe->std', gq_f32, wq_f32)
              + jnp.einsum('sjte,jde->std', gk_f32, wk_f32)
              + jnp.einsum('sjte,jde->std', gv_f32, wv_f32))
    return dx_f32.astype(jnp.bfloat16), dw_q, dw_k, dw_v, dw_o
```

```python
import functools

import jax
import jax.numpy as jnp
from jax import lax
from jax.experimental import pallas as pl
from jax.experimental.pallas import tpu as pltpu
from jax.sharding import PartitionSpec as P

MESH = pl.DeviceIdType.MESH
BF16 = jnp.bfloat16
F32 = jnp.float32
STRIDES = (1, 4, 16)
ORDERS = ((0, 1, 2), (1, 2, 0), (2, 0, 1))
NS = 6
W = 384


def tdot(a, b):
    return lax.dot_general(a, b, (((0,), (0,)), ((), ())), preferred_element_type=F32)


class Ring:
    def __init__(self, bufs, recvs, send_sem, recv_sem):
        self.bufs, self.recvs, self.send_sem, self.recv_sem = bufs, recvs, send_sem, recv_sem
        d = lax.axis_index('data')
        self.d = d
        self.coord = (d % 4, (d // 4) % 4, d // 16)

    def nbr(self, ax, delta):
        c = self.coord[ax]
        return self.d + ((c + delta + 4) % 4 - c) * STRIDES[ax]

    def barrier(self):
        sem = pltpu.get_barrier_semaphore()
        for ax in range(3):
            for delta in (1, -1):
                pl.semaphore_signal(sem, inc=1, device_id={'data': self.nbr(ax, delta)}, device_id_type=MESH)
        pl.semaphore_wait(sem, 6)

    def geom(self, s, p):
        ax = ORDERS[s // 2][p]
        sg = 1 if s % 2 == 0 else -1
        c = self.coord[ax]
        return ax, sg, c, (c + 2) % 4, (c + sg + 4) % 4, (c - sg + 4) % 4

    def msg(self, s, p, n):
        ax, sg, c, opp, fwd, back = self.geom(s, p)
        part = (opp, back, fwd)[n]
        to = (sg, -sg, sg)[n]
        return pltpu.make_async_remote_copy(
            src_ref=self.bufs[p].at[s, part], dst_ref=self.recvs[p].at[s, n],
            send_sem=self.send_sem.at[s, p, n], recv_sem=self.recv_sem.at[s, p, n],
            device_id={'data': self.nbr(ax, to)}, device_id_type=MESH)

    def start(self, s, p):
        self.msg(s, p, 0).start()
        self.msg(s, p, 1).start()

    def middle(self, s, p):
        fwd = self.geom(s, p)[4]
        self.msg(s, p, 0).wait_recv()
        buf, rcv = self.bufs[p], self.recvs[p]

        def add(*ix):
            buf[(s, fwd) + ix] = (buf[(s, fwd) + ix].astype(F32) + rcv[(s, 0) + ix].astype(F32)).astype(BF16)
        self.over(p, add)
        self.msg(s, p, 2).start()

    def over(self, p, f):
        if p == 2:
            f()
        elif p == 1:
            def body(i, _):
                f(i)
                return 0
            lax.fori_loop(0, 4, body, 0)
        else:
            def body(i, _):
                f(i // 4, i % 4)
                return 0
            lax.fori_loop(0, 16, body, 0)

    def finish(self, s, p):
        c = self.geom(s, p)[2]
        self.msg(s, p, 1).wait_recv()
        self.msg(s, p, 2).wait_recv()
        buf, rcv = self.bufs[p], self.recvs[p]

        def total(*ix):
            return buf[(s, c) + ix].astype(F32) + rcv[(s, 1) + ix].astype(F32) + rcv[(s, 2) + ix].astype(F32)
        if p == 2:
            return total()
        nxt = self.bufs[p + 1]

        def put(*ix):
            nxt[(s,) + ix] = total(*ix).astype(BF16)
        self.over(p, put)

    def drain(self):
        for s in range(NS):
            for p in range(3):
                for n in range(3):
                    self.msg(s, p, n).wait_send()


def grad_kernel(x, dy, dq, o, dkv, dwq_out, dwo_out, dwk_out, dwv_out,
                b0, b1, b2, r0, r1, r2, send_sem, recv_sem):
    ring = Ring((b0, b1, b2), (r0, r1, r2), send_sem, recv_sem)
    ring.barrier()
    m = lax.axis_index('model')

    def wo_block(i, _):
        v = tdot(dy[:, pl.ds(pl.multiple_of(i * 256, 256), 256)], o[...]).astype(BF16)
        for j in range(8):
            zc, yc, xc = i // 2, (i % 2) * 2 + j // 4, j % 4
            rows = v[j * 32:(j + 1) * 32]
            b0[2, yc, zc, xc] = rows[:, 0:384]
            b0[3, yc, zc, xc] = rows[:, 384:768]
            b0[5, zc, xc, yc, :, 0:256] = rows[:, 768:1024]
        return 0

    def wq_block(i, _):
        v = tdot(x[:, pl.ds(pl.multiple_of(i * 256, 256), 256)], dq[...]).astype(BF16)
        for j in range(8):
            zc, yc, xc = i // 2, (i % 2) * 2 + j // 4, j % 4
            rows = v[j * 32:(j + 1) * 32]
            b0[0, xc, yc, zc] = rows[:, 0:384]
            b0[1, xc, yc, zc] = rows[:, 384:768]
            b0[4, zc, xc, yc, :, 0:256] = rows[:, 768:1024]
        return 0

    def wkv_block(i, _):
        v = tdot(x[:, pl.ds(pl.multiple_of(m * 1024 + i * 256, 256), 256)], dkv[...]).astype(BF16)
        for j in range(16):
            rows = v[j * 16:(j + 1) * 16]
            for s, c0 in ((4, 0), (5, 256)):
                b0[s, i, j % 4, j // 4, 0:16, 256:384] = rows[:, c0:c0 + 128]
                b0[s, i, j % 4, j // 4, 16:32, 256:384] = rows[:, c0 + 128:c0 + 256]
        return 0

    lax.fori_loop(0, 8, wo_block, 0)
    for s in (2, 3):
        ring.start(s, 0)
    lax.fori_loop(0, 8, wq_block, 0)
    for s in (0, 1):
        ring.start(s, 0)
    lax.fori_loop(0, 4, wkv_block, 0)
    for s in (4, 5):
        ring.start(s, 0)
    order = (2, 3, 0, 1, 4, 5)
    for s in order:
        ring.middle(s, 0)
    for p in (1, 2):
        for s in order:
            ring.finish(s, p - 1)
            ring.start(s, p)
        for s in order:
            ring.middle(s, p)
    for s in order:
        v = ring.finish(s, 2)
        if s in (0, 1):
            dwq_out[:, s * 384:(s + 1) * 384] = v
        elif s in (2, 3):
            dwo_out[:, (s - 2) * 384:(s - 1) * 384] = v
        else:
            main, kv = (dwq_out, dwk_out) if s == 4 else (dwo_out, dwv_out)
            main[:, 768:1024] = v[:, 0:256]
            kv[:, 0:128] = v[0:16, 256:384]
            kv[:, 128:256] = v[16:32, 256:384]
    ring.drain()


def weight_grads(x, dy, dq, o, dkv):
    vmem = pl.BlockSpec(memory_space=pltpu.VMEM)
    return pl.pallas_call(
        grad_kernel,
        out_shape=(jax.ShapeDtypeStruct((32, 1024), F32), jax.ShapeDtypeStruct((32, 1024), F32),
                   jax.ShapeDtypeStruct((16, 256), F32), jax.ShapeDtypeStruct((16, 256), F32)),
        in_specs=[vmem] * 5, out_specs=[vmem] * 4,
        scratch_shapes=[
            pltpu.VMEM((NS, 4, 4, 4, 32, W), BF16), pltpu.VMEM((NS, 4, 4, 32, W), BF16), pltpu.VMEM((NS, 4, 32, W), BF16),
            pltpu.VMEM((NS, 3, 4, 4, 32, W), BF16), pltpu.VMEM((NS, 3, 4, 32, W), BF16), pltpu.VMEM((NS, 3, 32, W), BF16),
            pltpu.SemaphoreType.DMA((NS, 3, 3)), pltpu.SemaphoreType.DMA((NS, 3, 3))],
        compiler_params=pltpu.CompilerParams(collective_id=0, has_side_effects=True, vmem_limit_bytes=62 * 2 ** 20),
        cost_estimate=pl.CostEstimate(flops=10 ** 10, bytes_accessed=2 * 10 ** 7, transcendentals=0),
    )(x, dy, dq, o, dkv)


def solution(mesh):
    tok_spec = P(('pod', 'data'), 'model', None)
    swap = [(0, 1), (1, 0)]

    def device_step(x_loc, dy_loc, w_q, w_k, w_v, w_o):
        x_loc, dy_loc = x_loc[0], dy_loc[0]
        scale = w_k.shape[2] ** -0.5
        m = lax.axis_index('model')

        def gather(v):
            other = lax.ppermute(v, 'model', swap)
            return jnp.where(m == 0, jnp.concatenate([v, other]), jnp.concatenate([other, v]))
        x = gather(x_loc)
        dy = gather(dy_loc)
        w_kv = jnp.stack([w_k[0], w_v[0]])
        seq = x.shape[0]
        causal = lax.broadcasted_iota(jnp.int32, (seq, seq), 0) >= lax.broadcasted_iota(jnp.int32, (seq, seq), 1)
        q = jnp.einsum('td,dhe->hte', x, w_q, preferred_element_type=F32).astype(BF16)
        kv = jnp.einsum('td,nde->nte', x, w_kv, preferred_element_type=F32).astype(BF16)
        k, v = kv[0], kv[1]
        scores = jnp.einsum('hqe,ke->hqk', q, k, preferred_element_type=F32) * scale
        prob = jax.nn.softmax(jnp.where(causal, scores, -jnp.inf), axis=-1)
        prob_bf = prob.astype(BF16)
        o = jnp.einsum('hqk,ke->hqe', prob_bf, v, preferred_element_type=F32).astype(BF16)
        do = jnp.einsum('td,hed->hte', dy, w_o, preferred_element_type=F32).astype(BF16)
        dp = jnp.einsum('hqe,ke->hqk', do, v, preferred_element_type=F32)
        delta = jnp.einsum('hqe,hqe->hq', do, o, preferred_element_type=F32)
        ds = (prob * (dp - delta[..., None])).astype(BF16)
        dq = (jnp.einsum('hqk,ke->hqe', ds, k, preferred_element_type=F32) * scale).astype(BF16)
        dk = jnp.einsum('hqk,hqe->ke', ds, q, preferred_element_type=F32) * scale
        dv = jnp.einsum('hqk,hqe->ke', prob_bf, do, preferred_element_type=F32)
        dkv = jnp.concatenate([dk, dv], axis=1)
        dkv = (dkv + lax.ppermute(dkv, 'model', swap)).astype(BF16)
        dkv_own = lax.dynamic_slice_in_dim(dkv, m * (seq // 2), seq // 2, 0)
        dxp = jnp.einsum('hte,dhe->td', dq, w_q, preferred_element_type=F32)
        own = lax.dynamic_slice_in_dim(dxp, m * (seq // 2), seq // 2, 0)
        away = lax.dynamic_slice_in_dim(dxp, (1 - m) * (seq // 2), seq // 2, 0)
        dx = own + lax.ppermute(away, 'model', swap) + jnp.einsum(
            'te,de->td', dkv_own, jnp.concatenate([w_k[0], w_v[0]], axis=1), preferred_element_type=F32)
        flat = lambda a: a.transpose(1, 0, 2).reshape(seq, -1)
        dwq, dwo, dwk, dwv = weight_grads(x, dy, flat(dq), flat(o), dkv)
        heads = w_q.shape[1]
        return (dx.astype(BF16)[None], dwq.reshape(32, heads, -1), dwk, dwv,
                dwo.T.reshape(heads, -1, 32))

    kv_rows = P(('pod', 'model', 'data'), None)
    return jax.shard_map(device_step, mesh=mesh,
                         in_specs=(tok_spec, tok_spec, P(None, 'model', None), P(), P(), P('model', None, None)),
                         out_specs=(tok_spec, P(('pod', 'data'), 'model', None), kv_rows, kv_rows, P(('pod', 'model'), None, 'data')),
                         check_vma=False)
```

```python
import jax
import jax.numpy as jnp
from jax import lax
from jax.experimental import pallas as pl
from jax.experimental.pallas import tpu as pltpu
from jax.sharding import PartitionSpec as P

MESH = pl.DeviceIdType.MESH
BF16 = jnp.bfloat16
F32 = jnp.float32
NS = 6
NG = 3
SIZES = (16, 4, 1)
SEQ, HALF, D, E, NH = 1024, 512, 2048, 256, 4
CD = E ** -0.5
LOG2E = 1.4426950408889634


def nn(a, b):
    return lax.dot_general(a, b, (((1,), (0,)), ((), ())), preferred_element_type=F32)


def nt(a, b):
    return lax.dot_general(a, b, (((1,), (1,)), ((), ())), preferred_element_type=F32)


def tn(a, b):
    return lax.dot_general(a, b, (((0,), (0,)), ((), ())), preferred_element_type=F32)


def loop(n, f):
    def body(i, _):
        f(i)
        return 0
    lax.fori_loop(0, n, body, 0)


def pick(i, a, b, c):
    return a * ((1 - i) * (2 - i) // 2) + b * (i * (2 - i)) + c * (i * (i - 1) // 2)


def slot(s, xc, yc, zc):
    k = s // 2
    return pick(k, xc * 16 + yc * 4 + zc, yc * 16 + zc * 4 + xc, zc * 16 + xc * 4 + yc)


class Ring:
    def __init__(self, bufs, recvs, send_sem, recv_sem):
        self.bufs, self.recvs, self.send_sem, self.recv_sem = bufs, recvs, send_sem, recv_sem
        d = lax.axis_index('data')
        self.d = d
        self.coord = (d % 4, (d // 4) % 4, d // 16)

    def greet(self, sem):
        for ax in range(3):
            for delta in (1, -1):
                c = self.coord[ax]
                to = self.d + ((c + delta + 4) % 4 - c) * 4 ** ax
                pl.semaphore_signal(sem, inc=1, device_id={'data': to}, device_id_type=MESH)

    def geom(self, s, p):
        ax = (s // 2 + p) % 3
        sg = 1 - 2 * (s % 2)
        c = pick(ax, *self.coord)
        stride = pick(ax, 1, 4, 16)
        return c, (c + 2) % 4, (c + sg + 4) % 4, (c - sg + 4) % 4, stride

    def msg(self, g, s, p, n):
        c, opp, fwd, back, stride = self.geom(s, p)
        part = (opp, back, fwd)[n]
        to = self.d + ((fwd, back, fwd)[n] - c) * stride
        size = SIZES[p]
        return pltpu.make_async_remote_copy(
            src_ref=self.bufs[p].at[g, s, pl.ds(part * size, size)], dst_ref=self.recvs[p].at[g, s, n],
            send_sem=self.send_sem.at[g, s, p, n], recv_sem=self.recv_sem.at[g, s, p, n],
            device_id={'data': to}, device_id_type=MESH)

    def start_one(self, g, s, p):
        self.msg(g, s, p, 0).start()
        self.msg(g, s, p, 1).start()

    def start(self, g):
        loop(NS, lambda s: self.start_one(g, s, 0))

    def middle(self, g, p):
        buf, rcv, size = self.bufs[p], self.recvs[p], SIZES[p]

        def one(s):
            fwd = self.geom(s, p)[2]
            self.msg(g, s, p, 0).wait_recv()

            def add(i):
                buf[g, s, fwd * size + i] = (buf[g, s, fwd * size + i].astype(F32) + rcv[g, s, 0, i].astype(F32)).astype(BF16)
            loop(size, add)
            self.msg(g, s, p, 2).start()
        loop(NS, one)

    def finish(self, g, p, out=None):
        buf, rcv, size = self.bufs[p], self.recvs[p], SIZES[p]

        def one(s):
            c = self.geom(s, p)[0]
            self.msg(g, s, p, 1).wait_recv()
            self.msg(g, s, p, 2).wait_recv()

            def total(i):
                v = buf[g, s, c * size + i].astype(F32) + rcv[g, s, 1, i].astype(F32) + rcv[g, s, 2, i].astype(F32)
                if p == 2:
                    out[g, s] = v
                else:
                    self.bufs[p + 1][g, s, i] = v.astype(BF16)
            loop(size, total)
            if p < 2:
                self.start_one(g, s, p + 1)
        loop(NS, one)

    def drain(self):
        def one(s):
            for g in range(NG):
                for p in range(3):
                    for n in range(3):
                        self.msg(g, s, p, n).wait_send()
        loop(NS, one)


def layer_kernel(x_hbm, dy_hbm, wq_hbm, wk_hbm, wv_hbm, wo_hbm, dx_hbm, out,
                 x, dy, wq, wkv, wo, q, do, kv, kvt, ot, dqt, dq, dkv, dkv_in, dkvb, dx_in,
                 b0, b1, b2, r0, r1, r2, load_sem, pair_send, pair_recv, send_sem, recv_sem):
    m = lax.axis_index('model')
    ring = Ring((b0, b1, b2), (r0, r1, r2), send_sem, recv_sem)
    own = pl.ds(pl.multiple_of(m * HALF, HALF), HALF)
    away = pl.ds(pl.multiple_of((1 - m) * HALF, HALF), HALF)

    def load(src, dst, i):
        return pltpu.make_async_copy(src, dst, load_sem.at[i])

    def push(src, dst, i):
        return pltpu.make_async_remote_copy(src_ref=src, dst_ref=dst, send_sem=pair_send.at[i], recv_sem=pair_recv.at[i],
                                            device_id={'model': 1 - m}, device_id_type=MESH)
    loads = [load(x_hbm, x.at[own], 0), load(wq_hbm, wq, 1), load(wk_hbm, wkv.at[:, 0:E], 2), load(wv_hbm, wkv.at[:, E:2 * E], 3),
             load(dy_hbm, dy.at[own], 4), load(wo_hbm, wo, 5)]
    for c in loads:
        c.start()
    sem = pltpu.get_barrier_semaphore()
    ring.greet(sem)
    pl.semaphore_signal(sem, inc=1, device_id={'model': 1 - m}, device_id_type=MESH)
    pl.semaphore_wait(sem, 7)
    push_x = push(x_hbm, x.at[own], 0)
    push_dy = push(dy_hbm, dy.at[own], 1)
    push_x.start()
    push_dy.start()
    dkv[...] = jnp.zeros_like(dkv)

    def project_x(rows):
        def head(h):
            cols = pl.ds(pl.multiple_of(h * E, E), E)
            q[h, rows] = nn(x[rows], wq[:, cols]).astype(BF16)
        loop(NH, head)

        def kv_part(i):
            cols = pl.ds(pl.multiple_of(i * E, E), E)
            kv[rows, cols] = nn(x[rows], wkv[:, cols]).astype(BF16)
        loop(2, kv_part)

    def project_dy(rows):
        def head(h):
            do[h, rows] = nt(dy[rows], wo[pl.ds(pl.multiple_of(h * E, E), E)]).astype(BF16)
        loop(NH, head)
    for c in loads[:4]:
        c.wait()
    project_x(own)
    loads[4].wait()
    loads[5].wait()
    project_dy(own)
    push_x.wait_recv()
    project_x(away)
    push_dy.wait_recv()
    project_dy(away)

    def turn(i):
        cols = pl.ds(pl.multiple_of(i * 256, 256), 256)
        kvt[0:E, cols] = kv[cols, 0:E].T
        kvt[E:2 * E, cols] = kv[cols, E:2 * E].T
    loop(4, turn)

    def attend(h, j):
        n = (j + 1) * 256
        rows = slice(j * 256, n)
        qb = q[h, rows]
        dob = do[h, rows]
        st = nt(kv[0:n, 0:E], qb)
        keep = lax.broadcasted_iota(jnp.int32, (256, 256), 0) <= lax.broadcasted_iota(jnp.int32, (256, 256), 1)
        diag = jnp.where(keep, st[n - 256:n], -jnp.inf)
        st = diag if j == 0 else jnp.concatenate([st[0:n - 256], diag], axis=0)
        top = jnp.max(st, axis=0, keepdims=True)
        pt = jnp.exp2((st - top) * (CD * LOG2E))
        pt = pt * (1.0 / jnp.sum(pt, axis=0, keepdims=True))
        pb = pt.astype(BF16)
        ob = nn(kvt[E:2 * E, 0:n], pb).astype(BF16)
        ot[:, rows] = ob
        delta = jnp.sum(dob.T.astype(F32) * ob.astype(F32), axis=0, keepdims=True)
        dpt = nt(kv[0:n, E:2 * E], dob)
        dst = (pt * (dpt - delta)).astype(BF16)
        dqb = (nn(kvt[0:E, 0:n], dst) * CD).astype(BF16)
        dqt[:, rows] = dqb
        dq[rows, pl.ds(pl.multiple_of(h * E, E), E)] = dqb.T
        dkv[0:n, 0:E] += nn(dst, qb)
        dkv[0:n, E:2 * E] += nn(pb, dob)

    def store_tiles(t, v, i):
        for u in range(2):
            tile = t + u
            g, s = tile // NS, tile % NS
            for j in range(8):
                at = slot(s, j % 4, (i % 2) * 2 + j // 4, i // 2)
                b0[g, s, at] = v[j * 32:(j + 1) * 32, u * 128:(u + 1) * 128]

    def weight_grad(lhs, rhs, t):
        def block(i):
            v = nn(lhs[...], rhs[:, pl.ds(pl.multiple_of(i * 256, 256), 256)]).astype(BF16).T
            store_tiles(t, v, i)
        loop(8, block)

    def at_head(h, hh, f):
        @pl.when(h == hh)
        def _():
            f()

    def head_step(h):
        attend(h, 0)
        at_head(h, 3, lambda: ring.finish(0, 1))
        attend(h, 1)
        at_head(h, 2, lambda: ring.middle(0, 0))
        at_head(h, 3, lambda: ring.middle(1, 0))
        attend(h, 2)
        at_head(h, 3, lambda: ring.middle(0, 2))
        attend(h, 3)
        weight_grad(ot, dy, h * 4)
        at_head(h, 1, lambda: ring.start(0))
        at_head(h, 2, lambda: ring.finish(0, 0))
        at_head(h, 3, lambda: ring.finish(0, 2, out))
        weight_grad(dqt, x, h * 4 + 2)
        at_head(h, 2, lambda: ring.start(1))
        at_head(h, 2, lambda: ring.middle(0, 1))
        at_head(h, 3, lambda: ring.finish(1, 0))
    loop(NH, head_step)

    push_kv = push(dkv, dkv_in, 2)
    push_kv.start()
    def dx_away(i):
        cols = pl.ds(pl.multiple_of(i * 256, 256), 256)
        wo[0:HALF, cols] = nt(dq[away], wq[cols]).astype(BF16)
    push_kv.wait_recv()

    def kv_sum(i):
        rows = pl.ds(pl.multiple_of(i * 128, 128), 128)
        v = dkv[rows] + dkv_in[rows]
        dkvb[rows, 0:E] = (v[:, 0:E] * CD).astype(BF16)
        dkvb[rows, E:2 * E] = v[:, E:2 * E].astype(BF16)
    loop(8, kv_sum)

    def kv_block(i):
        v = tn(x[:, pl.ds(pl.multiple_of(m * 1024 + i * 256, 256), 256)], dkvb[...]).astype(BF16)
        for j in range(16):
            rows = v[j * 16:(j + 1) * 16]
            for u in range(2):
                at = slot(4 + u, j % 4, j // 4, i)
                b0[2, 4 + u, at, 0:16] = rows[:, u * E:u * E + 128]
                b0[2, 4 + u, at, 16:32] = rows[:, u * E + 128:u * E + 256]
    loop(4, kv_block)
    ring.start(2)
    ring.middle(1, 1)
    loop(8, dx_away)
    push_dx = push(wo.at[pl.ds(0, HALF)], dx_in, 3)
    push_dx.start()
    ring.middle(2, 0)
    ring.finish(1, 1)

    def dx_own(i):
        cols = pl.ds(pl.multiple_of(i * 256, 256), 256)
        v = nt(dq[own], wq[cols]) + nt(dkvb[own], wkv[cols])
        wo[HALF:SEQ, cols] = (v + dx_in[:, cols].astype(F32)).astype(BF16)
    push_dx.wait_recv()
    loop(8, dx_own)
    store_dx = load(wo.at[pl.ds(HALF, HALF)], dx_hbm, 6)
    store_dx.start()
    ring.middle(1, 2)
    ring.finish(2, 0)
    ring.finish(1, 2, out)
    ring.middle(2, 1)
    ring.finish(2, 1)
    ring.middle(2, 2)
    ring.finish(2, 2, out)
    ring.drain()
    for c in (push_x, push_dy, push_kv, push_dx):
        c.wait_send()
    store_dx.wait()


def layer(x, dy, wq, wk, wv, wo):
    hbm = pl.BlockSpec(memory_space=pl.ANY)
    dma = pltpu.SemaphoreType.DMA
    bf = lambda *shape: pltpu.VMEM(shape, BF16)
    return pl.pallas_call(
        layer_kernel,
        out_shape=(jax.ShapeDtypeStruct((HALF, D), BF16), jax.ShapeDtypeStruct((NG, NS, 32, 128), F32)),
        in_specs=[hbm] * 6, out_specs=[hbm, pl.BlockSpec(memory_space=pltpu.VMEM)],
        scratch_shapes=[
            bf(SEQ, D), bf(SEQ, D), bf(D, NH * E), bf(D, 2 * E), bf(NH * E, D),
            bf(NH, SEQ, E), bf(NH, SEQ, E), bf(SEQ, 2 * E), bf(2 * E, SEQ), bf(E, SEQ), bf(E, SEQ), bf(SEQ, NH * E),
            pltpu.VMEM((SEQ, 2 * E), F32), pltpu.VMEM((SEQ, 2 * E), F32), bf(SEQ, 2 * E), bf(HALF, D),
            bf(NG, NS, 64, 32, 128), bf(NG, NS, 16, 32, 128), bf(NG, NS, 4, 32, 128),
            bf(NG, NS, 3, 16, 32, 128), bf(NG, NS, 3, 4, 32, 128), bf(NG, NS, 3, 1, 32, 128),
            dma((7,)), dma((4,)), dma((4,)), dma((NG, NS, 3, 3)), dma((NG, NS, 3, 3))],
        compiler_params=pltpu.CompilerParams(collective_id=0, has_side_effects=True, vmem_limit_bytes=67043328),
        cost_estimate=pl.CostEstimate(flops=3 * 10 ** 10, bytes_accessed=2 * 10 ** 7, transcendentals=0),
    )(x, dy, wq, wk, wv, wo)


def solution(mesh):
    tok_spec = P(('pod', 'data'), 'model', None)

    def device_step(x_loc, dy_loc, w_q, w_k, w_v, w_o):
        dx, out = layer(x_loc[0], dy_loc[0], w_q.reshape(D, NH * E), w_k[0], w_v[0], w_o.reshape(NH * E, D))
        tiles = out.reshape(NG * NS, 32, 128)
        heads = tiles[0:16].reshape(NH, 2, 2, 32, 128)
        dwo = heads[:, 0].transpose(0, 1, 3, 2).reshape(NH, E, 32)
        dwq = heads[:, 1].transpose(2, 0, 1, 3).reshape(32, NH, E)
        kv = tiles[16:18].reshape(2, 2, 16, 128).transpose(0, 2, 1, 3).reshape(2, 16, E)
        return dx[None], dwq, kv[0], kv[1], dwo

    kv_rows = P(('pod', 'model', 'data'), None)
    return jax.shard_map(device_step, mesh=mesh,
                         in_specs=(tok_spec, tok_spec, P(None, 'model', None), P(), P(), P('model', None, None)),
                         out_specs=(tok_spec, P(('pod', 'data'), 'model', None), kv_rows, kv_rows, P(('pod', 'model'), None, 'data')),
                         check_vma=False)
```

```python
import jax
import jax.numpy as jnp
from jax import lax
from jax.experimental import pallas as pl
from jax.experimental.pallas import tpu as pltpu
from jax.sharding import PartitionSpec as P

MESH = pl.DeviceIdType.MESH
BF16 = jnp.bfloat16
F32 = jnp.float32
NT = 18
SIZES = (16, 4, 1)
GROUPS = ((0, 4), (4, 8), (8, 12), (12, 16), (16, 18))
SEQ, HALF, D, E, NH = 1024, 512, 2048, 256, 4
CD = E ** -0.5
LOG2E = 1.4426950408889634


def nn(a, b):
    return lax.dot_general(a, b, (((1,), (0,)), ((), ())), preferred_element_type=F32)


def nt(a, b):
    return lax.dot_general(a, b, (((1,), (1,)), ((), ())), preferred_element_type=F32)


def tn(a, b):
    return lax.dot_general(a, b, (((0,), (0,)), ((), ())), preferred_element_type=F32)


def loop(n, f, start=0):
    def body(i, _):
        f(i)
        return 0
    lax.fori_loop(start, n, body, 0)


def block(i, size):
    return pl.ds(pl.multiple_of(i * size, size), size)


def pick(i, a, b, c):
    return a * ((1 - i) * (2 - i) // 2) + b * (i * (2 - i)) + c * (i * (i - 1) // 2)


def slot(t, xc, yc, zc):
    return pick((t // 2) % 3, xc * 16 + yc * 4 + zc, yc * 16 + zc * 4 + xc, zc * 16 + xc * 4 + yc)


class Ring:
    def __init__(self, bufs, recvs, send_sem, recv_sem, store):
        self.bufs, self.recvs, self.send_sem, self.recv_sem, self.store = bufs, recvs, send_sem, recv_sem, store
        d = lax.axis_index('data')
        self.d = d
        self.coord = (d % 4, (d // 4) % 4, d // 16)

    def greet(self, sem):
        for ax in range(3):
            for delta in (1, -1):
                c = self.coord[ax]
                to = self.d + ((c + delta + 4) % 4 - c) * 4 ** ax
                pl.semaphore_signal(sem, inc=1, device_id={'data': to}, device_id_type=MESH)

    def geom(self, t, p):
        ax = ((t // 2) % 3 + p) % 3
        sg = 1 - 2 * (t % 2)
        c = pick(ax, *self.coord)
        stride = pick(ax, 1, 4, 16)
        return c, (c + 2) % 4, (c + sg + 4) % 4, (c - sg + 4) % 4, stride

    def msg(self, t, p, n):
        c, opp, fwd, back, stride = self.geom(t, p)
        part = (opp, back, fwd)[n]
        to = self.d + ((fwd, back, fwd)[n] - c) * stride
        size = SIZES[p]
        return pltpu.make_async_remote_copy(
            src_ref=self.bufs[p].at[t, pl.ds(part * size, size)], dst_ref=self.recvs[p].at[t, n],
            send_sem=self.send_sem.at[t, p, n], recv_sem=self.recv_sem.at[t, p, n],
            device_id={'data': to}, device_id_type=MESH)

    def tiles(self, g, f):
        lo, hi = GROUPS[g]
        loop(hi, f, lo)

    def start_one(self, t, p):
        self.msg(t, p, 0).start()
        self.msg(t, p, 1).start()

    def start(self, g):
        self.tiles(g, lambda t: self.start_one(t, 0))

    def chunks(self, p, f):
        step = min(SIZES[p], 4)
        if SIZES[p] == step:
            f(0, step)
        else:
            loop(SIZES[p] // step, lambda i: f(i * step, step))

    def middle(self, g, p):
        buf, rcv, size = self.bufs[p], self.recvs[p], SIZES[p]

        def one(t):
            fwd = self.geom(t, p)[2]
            self.msg(t, p, 0).wait_recv()

            def add(i, w):
                at = pl.ds(fwd * size + i, w)
                buf[t, at] = (buf[t, at].astype(F32) + rcv[t, 0, pl.ds(i, w)].astype(F32)).astype(BF16)
            self.chunks(p, add)
            self.msg(t, p, 2).start()
        self.tiles(g, one)

    def finish(self, g, p):
        buf, rcv, size = self.bufs[p], self.recvs[p], SIZES[p]

        def total(t, i, w):
            c = self.geom(t, p)[0]
            return (buf[t, pl.ds(c * size + i, w)].astype(F32) + rcv[t, 1, pl.ds(i, w)].astype(F32)
                    + rcv[t, 2, pl.ds(i, w)].astype(F32))

        def one(t):
            self.msg(t, p, 1).wait_recv()
            self.msg(t, p, 2).wait_recv()
            if p == 2:
                self.store(t, total(t, 0, 1)[0])
                return

            def put(i, w):
                self.bufs[p + 1][t, pl.ds(i, w)] = total(t, i, w).astype(BF16)
            self.chunks(p, put)
            self.start_one(t, p + 1)
        if p == 2:
            for t in range(*GROUPS[g]):
                one(t)
        else:
            self.tiles(g, one)

    def drain(self):
        def one(t):
            for p in range(3):
                for n in range(3):
                    self.msg(t, p, n).wait_send()
        loop(NT, one)


def layer_kernel(x_hbm, dy_hbm, wq_hbm, wk_hbm, wv_hbm, wo_hbm, dx_hbm, dwq_out, dwk_out, dwv_out, dwo_out,
                 x, dy, wq, wkv, wo, q, do, kv, kvt, ot, dqt, dq, dkv, dkv_in, dkvb, dx_in,
                 b0, b1, b2, r0, r1, r2, load_sem, pair_send, pair_recv, send_sem, recv_sem):
    m = lax.axis_index('model')

    def store(t, v):
        if t >= 16:
            out = (dwk_out, dwv_out)[t - 16]
            out[:, 0:128] = v[0:16]
            out[:, 128:256] = v[16:32]
        else:
            h, u = divmod(t, 4)
            cols = slice((u % 2) * 128, (u % 2) * 128 + 128)
            if u < 2:
                dwo_out[h, :, cols] = v
            else:
                dwq_out[:, h, cols] = v
    ring = Ring((b0, b1, b2), (r0, r1, r2), send_sem, recv_sem, store)
    own = block(m, HALF)
    away = block(1 - m, HALF)

    def load(src, dst, i):
        return pltpu.make_async_copy(src, dst, load_sem.at[i])

    def push(src, dst, i):
        return pltpu.make_async_remote_copy(src_ref=src, dst_ref=dst, send_sem=pair_send.at[i], recv_sem=pair_recv.at[i],
                                            device_id={'model': 1 - m}, device_id_type=MESH)
    loads = [load(x_hbm, x.at[own], 0), load(wq_hbm, wq, 1), load(wk_hbm, wkv.at[:, 0:E], 2), load(wv_hbm, wkv.at[:, E:2 * E], 3),
             load(dy_hbm, dy.at[own], 4), load(wo_hbm, wo, 5)]
    for c in loads:
        c.start()
    sem = pltpu.get_barrier_semaphore()
    ring.greet(sem)
    pl.semaphore_signal(sem, inc=1, device_id={'model': 1 - m}, device_id_type=MESH)
    dkv[...] = jnp.zeros_like(dkv)
    pl.semaphore_wait(sem, 7)
    push_x = push(x_hbm, x.at[own], 0)
    push_dy = push(dy_hbm, dy.at[own], 1)
    push_x.start()
    push_dy.start()

    def project_x(rows):
        def pair(i):
            for h in range(2):
                q[i * 2 + h, rows] = nn(x[rows], wq[:, block(i * 2 + h, E)]).astype(BF16)
        loop(NH // 2, pair)
        kv[rows] = nn(x[rows], wkv[...]).astype(BF16)

    def project_dy(rows):
        def pair(i):
            for h in range(2):
                do[i * 2 + h, rows] = nt(dy[rows], wo[block(i * 2 + h, E)]).astype(BF16)
        loop(NH // 2, pair)
    for c in loads[:4]:
        c.wait()
    project_x(own)
    loads[4].wait()
    loads[5].wait()
    project_dy(own)
    push_x.wait_recv()
    project_x(away)
    push_dy.wait_recv()
    project_dy(away)

    def turn(i):
        cols = block(i, 256)
        kvt[0:E, cols] = kv[cols, 0:E].T
        kvt[E:2 * E, cols] = kv[cols, E:2 * E].T
    loop(4, turn)

    def attend(h, j):
        n = (j + 1) * 256
        rows = slice(j * 256, n)
        qb = q[h, rows]
        dob = do[h, rows]
        st = nt(kv[0:n, 0:E], qb)
        dpt = nt(kv[0:n, E:2 * E], dob)
        yield
        keep = lax.broadcasted_iota(jnp.int32, (256, 256), 0) <= lax.broadcasted_iota(jnp.int32, (256, 256), 1)
        diag = jnp.where(keep, st[n - 256:n], -jnp.inf)
        st = diag if j == 0 else jnp.concatenate([st[0:n - 256], diag], axis=0)
        top = jnp.max(st, axis=0, keepdims=True)
        pt = jnp.exp2((st - top) * (CD * LOG2E))
        pt = pt * (1.0 / jnp.sum(pt, axis=0, keepdims=True))
        pb = pt.astype(BF16)
        yield
        ob = nn(kvt[E:2 * E, 0:n], pb).astype(BF16)
        ot[:, rows] = ob
        delta = jnp.sum(dob.T.astype(F32) * ob.astype(F32), axis=0, keepdims=True)
        dkv[0:n, E:2 * E] += nn(pb, dob)
        yield
        dst = (pt * (dpt - delta)).astype(BF16)
        yield
        dqb = (nn(kvt[0:E, 0:n], dst) * CD).astype(BF16)
        dqt[:, rows] = dqb
        dq[rows, block(h, E)] = dqb.T
        dkv[0:n, 0:E] += nn(dst, qb)
        yield

    def attention(h):
        todo = [attend(h, j) for j in (3, 2, 1, 0)]
        for tick in range(5 + 2 * 3):
            for b, stages in enumerate(todo):
                if 0 <= tick - 2 * b < 5:
                    next(stages)

    def store_tiles(t, v, i):
        for u in range(2):
            for j in range(8):
                at = slot(t + u, j % 4, (i % 2) * 2 + j // 4, i // 2)
                b0[t + u, at] = v[j * 32:(j + 1) * 32, u * 128:(u + 1) * 128]

    def weight_grads(h):
        def step(i):
            vo = nn(ot[...], dy[:, block(i, 512)]).astype(BF16).T
            vq = nn(dqt[...], x[:, block(i, 512)]).astype(BF16).T
            for u in range(2):
                store_tiles(h * 4, vo[u * 256:(u + 1) * 256], i * 2 + u)
                store_tiles(h * 4 + 2, vq[u * 256:(u + 1) * 256], i * 2 + u)
        loop(4, step)
    push_kv = push(dkv, dkv_in, 2)

    def after_attention(h):
        if h == 1:
            ring.middle(0, 0)
        if h == 2:
            ring.finish(0, 0)
            ring.middle(1, 0)
        if h == 3:
            push_kv.start()
            ring.finish(0, 1)
            ring.finish(1, 0)
            ring.middle(2, 0)

    def after_grads(h):
        ring.start(h)
        if h == 2:
            ring.middle(0, 1)
        if h == 3:
            ring.middle(0, 2)
            ring.middle(1, 1)

    def head_step(h):
        attention(h)
        for hh in range(1, NH):
            @pl.when(h == hh)
            def _():
                after_attention(hh)
        weight_grads(h)
        for hh in range(NH):
            @pl.when(h == hh)
            def _():
                after_grads(hh)
    loop(NH, head_step)

    push_kv.wait_recv()

    def kv_sum(i):
        rows = block(i, 128)
        v = dkv[rows] + dkv_in[rows]
        dkvb[rows, 0:E] = (v[:, 0:E] * CD).astype(BF16)
        dkvb[rows, E:2 * E] = v[:, E:2 * E].astype(BF16)
    loop(8, kv_sum)

    def kv_block(i):
        v = tn(x[:, block(m * 4 + i, 256)], dkvb[...]).astype(BF16)
        for j in range(16):
            rows = v[j * 16:(j + 1) * 16]
            for u in range(2):
                at = slot(16 + u, j % 4, j // 4, i)
                b0[16 + u, at, 0:16] = rows[:, u * E:u * E + 128]
                b0[16 + u, at, 16:32] = rows[:, u * E + 128:u * E + 256]
    loop(4, kv_block)
    ring.start(4)
    ring.finish(2, 0)
    ring.finish(0, 2)
    ring.finish(1, 1)
    ring.middle(3, 0)

    def dx_away(i):
        cols = block(i, 512)
        wo[0:HALF, cols] = nt(dq[away], wq[cols]).astype(BF16)
    loop(4, dx_away)
    push_dx = push(wo.at[pl.ds(0, HALF)], dx_in, 3)
    push_dx.start()
    ring.middle(1, 2)
    ring.middle(2, 1)
    ring.middle(4, 0)

    def dx_own(i):
        cols = block(i, 512)
        v = nt(dq[own], wq[cols]) + nt(dkvb[own], wkv[cols])
        wo[HALF:SEQ, cols] = (v + dx_in[:, cols].astype(F32)).astype(BF16)
    push_dx.wait_recv()
    loop(2, dx_own)
    ring.finish(2, 1)
    ring.finish(3, 0)
    ring.finish(1, 2)
    loop(4, dx_own, 2)
    store_dx = load(wo.at[pl.ds(HALF, HALF)], dx_hbm, 6)
    store_dx.start()
    ring.middle(2, 2)
    ring.finish(4, 0)
    ring.middle(3, 1)
    ring.finish(2, 2)
    ring.finish(3, 1)
    ring.middle(4, 1)
    ring.middle(3, 2)
    ring.finish(4, 1)
    ring.finish(3, 2)
    ring.middle(4, 2)
    ring.finish(4, 2)
    ring.drain()
    for c in (push_x, push_dy, push_kv, push_dx):
        c.wait_send()
    store_dx.wait()


def layer(x, dy, wq, wk, wv, wo):
    hbm = pl.BlockSpec(memory_space=pl.ANY)
    dma = pltpu.SemaphoreType.DMA
    bf = lambda *shape: pltpu.VMEM(shape, BF16)
    return pl.pallas_call(
        layer_kernel,
        out_shape=(jax.ShapeDtypeStruct((HALF, D), BF16), jax.ShapeDtypeStruct((32, NH, E), F32),
                   jax.ShapeDtypeStruct((16, E), F32), jax.ShapeDtypeStruct((16, E), F32), jax.ShapeDtypeStruct((NH, 32, E), F32)),
        in_specs=[hbm] * 6, out_specs=[hbm] + [pl.BlockSpec(memory_space=pltpu.VMEM)] * 4,
        scratch_shapes=[
            bf(SEQ, D), bf(SEQ, D), bf(D, NH * E), bf(D, 2 * E), bf(NH * E, D),
            bf(NH, SEQ, E), bf(NH, SEQ, E), bf(SEQ, 2 * E), bf(2 * E, SEQ), bf(E, SEQ), bf(E, SEQ), bf(SEQ, NH * E),
            pltpu.VMEM((SEQ, 2 * E), F32), pltpu.VMEM((SEQ, 2 * E), F32), bf(SEQ, 2 * E), bf(HALF, D),
            bf(NT, 64, 32, 128), bf(NT, 16, 32, 128), bf(NT, 4, 32, 128),
            bf(NT, 3, 16, 32, 128), bf(NT, 3, 4, 32, 128), bf(NT, 3, 1, 32, 128),
            dma((7,)), dma((4,)), dma((4,)), dma((NT, 3, 3)), dma((NT, 3, 3))],
        compiler_params=pltpu.CompilerParams(collective_id=0, has_side_effects=True, vmem_limit_bytes=67043328),
        cost_estimate=pl.CostEstimate(flops=3 * 10 ** 10, bytes_accessed=2 * 10 ** 7, transcendentals=0),
    )(x, dy, wq, wk, wv, wo)


def solution(mesh):
    tok_spec = P(('pod', 'data'), 'model', None)

    def device_step(x_loc, dy_loc, w_q, w_k, w_v, w_o):
        dx, dwq, dwk, dwv, dwo = layer(x_loc[0], dy_loc[0], w_q.reshape(D, NH * E), w_k[0], w_v[0], w_o.reshape(NH * E, D))
        return dx[None], dwq, dwk, dwv, dwo.transpose(0, 2, 1)

    kv_rows = P(('pod', 'model', 'data'), None)
    return jax.shard_map(device_step, mesh=mesh,
                         in_specs=(tok_spec, tok_spec, P(None, 'model', None), P(), P(), P('model', None, None)),
                         out_specs=(tok_spec, P(('pod', 'data'), 'model', None), kv_rows, kv_rows, P(('pod', 'model'), None, 'data')),
                         check_vma=False)
```

```python
import jax
import jax.numpy as jnp
from jax import lax
from jax.experimental import pallas as pl
from jax.experimental.pallas import tpu as pltpu
from jax.sharding import PartitionSpec as P

MESH = pl.DeviceIdType.MESH
BF16 = jnp.bfloat16
F32 = jnp.float32
NT = 18
SIZES = (16, 4, 1)
GROUPS = ((0, 4), (4, 8), (8, 12), (12, 16), (16, 18))
SEQ, HALF, D, E, NH = 1024, 512, 2048, 256, 4
CD = E ** -0.5
LOG2E = 1.4426950408889634


def nn(a, b):
    return lax.dot_general(a, b, (((1,), (0,)), ((), ())), preferred_element_type=F32)


def nt(a, b):
    return lax.dot_general(a, b, (((1,), (1,)), ((), ())), preferred_element_type=F32)


def tn(a, b):
    return lax.dot_general(a, b, (((0,), (0,)), ((), ())), preferred_element_type=F32)


def loop(n, f, start=0):
    def body(i, _):
        f(i)
        return 0
    lax.fori_loop(start, n, body, 0)


def block(i, size):
    return pl.ds(pl.multiple_of(i * size, size), size)


def pick(i, a, b, c):
    return a * ((1 - i) * (2 - i) // 2) + b * (i * (2 - i)) + c * (i * (i - 1) // 2)


def steps_of(t):
    k = (t // 2) % 3
    return pick(k, 16, 1, 4), pick(k, 4, 16, 1), pick(k, 1, 4, 16)


class Ring:
    def __init__(self, bufs, recvs, send_sem, recv_sem, store):
        self.bufs, self.recvs, self.send_sem, self.recv_sem, self.store = bufs, recvs, send_sem, recv_sem, store
        d = lax.axis_index('data')
        self.d = d
        self.coord = (d % 4, (d // 4) % 4, d // 16)

    def greet(self, sem):
        for ax in range(3):
            for delta in (1, -1, 2):
                c = self.coord[ax]
                to = self.d + ((c + delta + 4) % 4 - c) * 4 ** ax
                pl.semaphore_signal(sem, inc=1, device_id={'data': to}, device_id_type=MESH)

    def geom(self, t, p):
        ax = ((t // 2) % 3 + p) % 3
        sg = 1 - 2 * (t % 2)
        c = pick(ax, *self.coord)
        stride = pick(ax, 1, 4, 16)
        return c, (c + 2) % 4, (c + sg + 4) % 4, (c - sg + 4) % 4, stride

    def msg(self, t, p, n):
        c, opp, fwd, back, stride = self.geom(t, p)
        part = (opp, back, fwd)[n]
        to = part if p == 2 else (fwd, back, fwd)[n]
        to = self.d + (to - c) * stride
        size = SIZES[p]
        return pltpu.make_async_remote_copy(
            src_ref=self.bufs[p].at[t, pl.ds(part * size, size)], dst_ref=self.recvs[p].at[t, n],
            send_sem=self.send_sem.at[t, p, n], recv_sem=self.recv_sem.at[t, p, n],
            device_id={'data': to}, device_id_type=MESH)

    def tiles(self, g, f):
        lo, hi = GROUPS[g]
        loop(hi, f, lo)

    def start(self, g):
        for n in range(2):
            self.tiles(g, lambda t: self.msg(t, 0, n).start())

    def chunks(self, p, f):
        step = min(SIZES[p], 4)
        if SIZES[p] == step:
            f(0, step)
        else:
            loop(SIZES[p] // step, lambda i: f(i * step, step))

    def middle(self, g, p):
        buf, rcv, size = self.bufs[p], self.recvs[p], SIZES[p]

        def one(t):
            fwd = self.geom(t, p)[2]
            self.msg(t, p, 0).wait_recv()

            def add(i, w):
                at = pl.ds(fwd * size + i, w)
                buf[t, at] = (buf[t, at].astype(F32) + rcv[t, 0, pl.ds(i, w)].astype(F32)).astype(BF16)
            self.chunks(p, add)
            self.msg(t, p, 2).start()
        self.tiles(g, one)

    def finish(self, g, p):
        buf, rcv, size = self.bufs[p], self.recvs[p], SIZES[p]

        def total(t, i, w):
            c = self.geom(t, p)[0]
            v = buf[t, pl.ds(c * size + i, w)].astype(F32)
            for n in range(0 if p == 2 else 1, 3):
                v = v + rcv[t, n, pl.ds(i, w)].astype(F32)
            return v

        def one(t):
            for n in range(0 if p == 2 else 1, 3):
                self.msg(t, p, n).wait_recv()
            if p == 2:
                self.store(t, total(t, 0, 1)[0])
                return

            def put(i, w):
                self.bufs[p + 1][t, pl.ds(i, w)] = total(t, i, w).astype(BF16)
            self.chunks(p, put)
            self.msg(t, p + 1, 0).start()
        if p == 2:
            for t in range(*GROUPS[g]):
                one(t)
            return
        self.tiles(g, one)
        for n in range(1, 3 if p == 1 else 2):
            self.tiles(g, lambda t: self.msg(t, p + 1, n).start())

    def drain(self):
        def one(t):
            for p in range(3):
                for n in range(3):
                    self.msg(t, p, n).wait_send()
        loop(NT, one)


def layer_kernel(x_hbm, dy_hbm, wq_hbm, wk_hbm, wv_hbm, wo_hbm, dx_hbm, dwq_out, dwk_out, dwv_out, dwo_out,
                 x, dy, wq, wkv, wo, q, do, kv, kvt, ot, dqt, dq, dkv, dkv_in, dkvb, dx_in,
                 b0, b1, b2, r0, r1, r2, load_sem, pair_send, pair_recv, send_sem, recv_sem):
    m = lax.axis_index('model')

    def store(t, v):
        if t >= 16:
            out = (dwk_out, dwv_out)[t - 16]
            out[:, 0:128] = v[0:16]
            out[:, 128:256] = v[16:32]
        else:
            h, u = divmod(t, 4)
            cols = slice((u % 2) * 128, (u % 2) * 128 + 128)
            if u < 2:
                dwo_out[h, :, cols] = v
            else:
                dwq_out[:, h, cols] = v
    ring = Ring((b0, b1, b2), (r0, r1, r2), send_sem, recv_sem, store)
    own = block(m, HALF)
    away = block(1 - m, HALF)

    def load(src, dst, i):
        return pltpu.make_async_copy(src, dst, load_sem.at[i])

    def push(src, dst, i):
        return pltpu.make_async_remote_copy(src_ref=src, dst_ref=dst, send_sem=pair_send.at[i], recv_sem=pair_recv.at[i],
                                            device_id={'model': 1 - m}, device_id_type=MESH)
    loads = [load(x_hbm, x.at[own], 0), load(wq_hbm, wq, 1), load(wk_hbm, wkv.at[:, 0:E], 2), load(wv_hbm, wkv.at[:, E:2 * E], 3),
             load(dy_hbm, dy.at[own], 4), load(wo_hbm, wo, 5)]
    for c in loads:
        c.start()
    sem = pltpu.get_barrier_semaphore()
    ring.greet(sem)
    pl.semaphore_signal(sem, inc=1, device_id={'model': 1 - m}, device_id_type=MESH)
    dkv[...] = jnp.zeros_like(dkv)
    pl.semaphore_wait(sem, 10)
    push_x = push(x_hbm, x.at[own], 0)
    push_dy = push(dy_hbm, dy.at[own], 1)
    push_x.start()
    push_dy.start()

    def project_q(h, rows):
        q[h, rows] = nn(x[rows], wq[:, block(h, E)]).astype(BF16)

    def project_do(h, rows):
        do[h, rows] = nt(dy[rows], wo[block(h, E)]).astype(BF16)

    def project_kv(rows):
        kv[rows] = nn(x[rows], wkv[...]).astype(BF16)

    def project_x_own(i):
        for h in range(2):
            project_q(i * 2 + h, own)

    def project_dy_own(i):
        for h in range(2):
            project_do(i * 2 + h, own)
    for c in loads[:4]:
        c.wait()
    loop(2, project_x_own)
    project_kv(own)
    loads[4].wait()
    loads[5].wait()
    loop(2, project_dy_own)
    push_x.wait_recv()
    project_kv(away)
    project_q(0, away)
    push_dy.wait_recv()
    project_do(0, away)

    def turn(i):
        cols = block(i, 256)
        kvt[0:E, cols] = kv[cols, 0:E].T
        kvt[E:2 * E, cols] = kv[cols, E:2 * E].T
    loop(4, turn)

    def attend(h, j):
        n = (j + 1) * 256
        rows = slice(j * 256, n)
        qb = q[h, rows]
        dob = do[h, rows]
        st = nt(kv[0:n, 0:E], qb)
        dpt = nt(kv[0:n, E:2 * E], dob)
        yield
        keep = lax.broadcasted_iota(jnp.int32, (256, 256), 0) <= lax.broadcasted_iota(jnp.int32, (256, 256), 1)
        diag = jnp.where(keep, st[n - 256:n], -jnp.inf)
        st = diag if j == 0 else jnp.concatenate([st[0:n - 256], diag], axis=0)
        top = jnp.max(st, axis=0, keepdims=True)
        pt = jnp.exp2((st - top) * (CD * LOG2E))
        pt = pt * (1.0 / jnp.sum(pt, axis=0, keepdims=True))
        pb = pt.astype(BF16)
        yield
        ob = nn(kvt[E:2 * E, 0:n], pb).astype(BF16)
        ot[:, rows] = ob
        delta = jnp.sum(dob.T.astype(F32) * ob.astype(F32), axis=0, keepdims=True)
        dkv[0:n, E:2 * E] += nn(pb, dob)
        yield
        dst = (pt * (dpt - delta)).astype(BF16)
        yield
        dqb = (nn(kvt[0:E, 0:n], dst) * CD).astype(BF16)
        dqt[:, rows] = dqb
        dq[rows, block(h, E)] = dqb.T
        dkv[0:n, 0:E] += nn(dst, qb)
        yield

    def attention(h):
        todo = [attend(h, j) for j in (3, 2, 1, 0)]
        for tick in range(5 + 2 * 3):
            for b, stages in enumerate(todo):
                if 0 <= tick - 2 * b < 5:
                    next(stages)
            if tick == 1:
                project_q((h + 1) % NH, away)
            if tick == 5:
                project_do((h + 1) % NH, away)

    def store_tiles(t, v, i):
        sx, sy, sz = steps_of(t)
        base = (i % 2) * 2 * sy + (i // 2) * sz
        for j in range(8):
            at = base + (j % 4) * sx + (j // 4) * sy
            for u in range(2):
                b0[t + u, at] = v[j * 32:(j + 1) * 32, u * 128:(u + 1) * 128]

    def weight_grads(h, half):
        def step(i):
            vo = nn(ot[...], dy[:, block(i, 512)]).astype(BF16).T
            vq = nn(dqt[...], x[:, block(i, 512)]).astype(BF16).T
            for u in range(2):
                store_tiles(h * 4, vo[u * 256:(u + 1) * 256], i * 2 + u)
                store_tiles(h * 4 + 2, vq[u * 256:(u + 1) * 256], i * 2 + u)
        loop(half * 2 + 2, step, half * 2)
    push_kv = push(dkv, dkv_in, 2)

    def amid_grads(h):
        if h > 0:
            ring.middle(h - 1, 0)
        if h > 1:
            ring.finish(h - 2, 0)

    def after_grads(h):
        ring.start(h)
        if h == 3:
            ring.finish(0, 1)

    def at_head(h, f):
        for hh in range(NH):
            @pl.when(h == hh)
            def _():
                f(hh)

    def head_step(h):
        attention(h)

        @pl.when(h == NH - 1)
        def _():
            push_kv.start()
            ring.middle(0, 1)

        def half_step(half):
            weight_grads(h, half)

            @pl.when(half == 0)
            def _():
                at_head(h, amid_grads)

            @pl.when(half == 1)
            def _():
                at_head(h, after_grads)
        loop(2, half_step)
    loop(NH, head_step)

    push_kv.wait_recv()

    def kv_sum(i):
        rows = block(i, 128)
        v = dkv[rows] + dkv_in[rows]
        dkvb[rows, 0:E] = (v[:, 0:E] * CD).astype(BF16)
        dkvb[rows, E:2 * E] = v[:, E:2 * E].astype(BF16)
    loop(8, kv_sum)

    def kv_block(i):
        v = tn(x[:, block(m * 4 + i, 256)], dkvb[...]).astype(BF16)
        for j in range(16):
            rows = v[j * 16:(j + 1) * 16]
            at = i * 16 + (j % 4) * 4 + j // 4
            for u in range(2):
                b0[16 + u, at, 0:16] = rows[:, u * E:u * E + 128]
                b0[16 + u, at, 16:32] = rows[:, u * E + 128:u * E + 256]
    loop(4, kv_block)
    ring.start(4)
    ring.middle(1, 1)

    def dx_away(i):
        cols = block(i, 512)
        wo[0:HALF, cols] = nt(dq[away], wq[cols]).astype(BF16)
    loop(4, dx_away)
    push_dx = push(wo.at[pl.ds(0, HALF)], dx_in, 3)
    push_dx.start()
    ring.middle(3, 0)
    ring.finish(0, 2)
    ring.finish(1, 1)
    ring.finish(2, 0)

    def dx_own(i):
        cols = block(i, 512)
        v = nt(dq[own], wq[cols]) + nt(dkvb[own], wkv[cols])
        wo[HALF:SEQ, cols] = (v + dx_in[:, cols].astype(F32)).astype(BF16)
    push_dx.wait_recv()
    loop(2, dx_own)
    ring.middle(4, 0)
    ring.middle(2, 1)
    loop(4, dx_own, 2)
    store_dx = load(wo.at[pl.ds(HALF, HALF)], dx_hbm, 6)
    store_dx.start()
    ring.finish(1, 2)
    ring.finish(3, 0)
    ring.finish(2, 1)
    ring.finish(4, 0)
    ring.middle(3, 1)
    ring.finish(2, 2)
    ring.middle(4, 1)
    ring.finish(3, 1)
    ring.finish(4, 1)
    ring.finish(3, 2)
    ring.finish(4, 2)
    ring.drain()
    for c in (push_x, push_dy, push_kv, push_dx):
        c.wait_send()
    store_dx.wait()


def layer(x, dy, wq, wk, wv, wo):
    hbm = pl.BlockSpec(memory_space=pl.ANY)
    dma = pltpu.SemaphoreType.DMA
    bf = lambda *shape: pltpu.VMEM(shape, BF16)
    return pl.pallas_call(
        layer_kernel,
        out_shape=(jax.ShapeDtypeStruct((HALF, D), BF16), jax.ShapeDtypeStruct((32, NH, E), F32),
                   jax.ShapeDtypeStruct((16, E), F32), jax.ShapeDtypeStruct((16, E), F32), jax.ShapeDtypeStruct((NH, 32, E), F32)),
        in_specs=[hbm] * 6, out_specs=[hbm] + [pl.BlockSpec(memory_space=pltpu.VMEM)] * 4,
        scratch_shapes=[
            bf(SEQ, D), bf(SEQ, D), bf(D, NH * E), bf(D, 2 * E), bf(NH * E, D),
            bf(NH, SEQ, E), bf(NH, SEQ, E), bf(SEQ, 2 * E), bf(2 * E, SEQ), bf(E, SEQ), bf(E, SEQ), bf(SEQ, NH * E),
            pltpu.VMEM((SEQ, 2 * E), F32), pltpu.VMEM((SEQ, 2 * E), F32), bf(SEQ, 2 * E), bf(HALF, D),
            bf(NT, 64, 32, 128), bf(NT, 16, 32, 128), bf(NT, 4, 32, 128),
            bf(NT, 3, 16, 32, 128), bf(NT, 3, 4, 32, 128), bf(NT, 3, 1, 32, 128),
            dma((7,)), dma((4,)), dma((4,)), dma((NT, 3, 3)), dma((NT, 3, 3))],
        compiler_params=pltpu.CompilerParams(collective_id=0, has_side_effects=True, vmem_limit_bytes=67043328),
        cost_estimate=pl.CostEstimate(flops=3 * 10 ** 10, bytes_accessed=2 * 10 ** 7, transcendentals=0),
    )(x, dy, wq, wk, wv, wo)


def solution(mesh):
    tok_spec = P(('pod', 'data'), 'model', None)

    def device_step(x_loc, dy_loc, w_q, w_k, w_v, w_o):
        dx, dwq, dwk, dwv, dwo = layer(x_loc[0], dy_loc[0], w_q.reshape(D, NH * E), w_k[0], w_v[0], w_o.reshape(NH * E, D))
        return dx[None], dwq, dwk, dwv, dwo.transpose(0, 2, 1)

    kv_rows = P(('pod', 'model', 'data'), None)
    return jax.shard_map(device_step, mesh=mesh,
                         in_specs=(tok_spec, tok_spec, P(None, 'model', None), P(), P(), P('model', None, None)),
                         out_specs=(tok_spec, P(('pod', 'data'), 'model', None), kv_rows, kv_rows, P(('pod', 'model'), None, 'data')),
                         check_vma=False)
```

```python
import jax
import jax.numpy as jnp
from jax import lax
from jax.experimental import pallas as pl
from jax.experimental.pallas import tpu as pltpu
from jax.sharding import PartitionSpec as P

MESH = pl.DeviceIdType.MESH
BF16 = jnp.bfloat16
F32 = jnp.float32
NT = 18
SIZES = (16, 4, 1)
GROUPS = ((0, 4), (4, 8), (8, 12), (12, 16), (16, 18))
SEQ, HALF, D, E, NH = 1024, 512, 2048, 256, 4
CD = E ** -0.5
LOG2E = 1.4426950408889634


def nn(a, b):
    return lax.dot_general(a, b, (((1,), (0,)), ((), ())), preferred_element_type=F32)


def nt(a, b):
    return lax.dot_general(a, b, (((1,), (1,)), ((), ())), preferred_element_type=F32)


def tn(a, b):
    return lax.dot_general(a, b, (((0,), (0,)), ((), ())), preferred_element_type=F32)


def loop(n, f, start=0):
    def body(i, _):
        f(i)
        return 0
    lax.fori_loop(start, n, body, 0)


def block(i, size):
    return pl.ds(pl.multiple_of(i * size, size), size)


def pick(i, a, b, c):
    return a * ((1 - i) * (2 - i) // 2) + b * (i * (2 - i)) + c * (i * (i - 1) // 2)


def steps_of(t):
    k = (t // 2) % 3
    return pick(k, 16, 1, 4), pick(k, 4, 16, 1), pick(k, 1, 4, 16)


class Ring:
    def __init__(self, bufs, recvs, send_sem, recv_sem, store):
        self.bufs, self.recvs, self.send_sem, self.recv_sem, self.store = bufs, recvs, send_sem, recv_sem, store
        d = lax.axis_index('data')
        self.d = d
        self.coord = (d % 4, (d // 4) % 4, d // 16)

    def greet(self, sem):
        for ax in range(3):
            for delta in (1, -1, 2):
                c = self.coord[ax]
                to = self.d + ((c + delta + 4) % 4 - c) * 4 ** ax
                pl.semaphore_signal(sem, inc=1, device_id={'data': to}, device_id_type=MESH)

    def geom(self, t, p):
        ax = ((t // 2) % 3 + p) % 3
        sg = 1 - 2 * (t % 2)
        c = pick(ax, *self.coord)
        stride = pick(ax, 1, 4, 16)
        return c, (c + 2) % 4, (c + sg + 4) % 4, (c - sg + 4) % 4, stride

    def direct(self, g, p):
        return p == 2 or (p == 1 and g >= 3)

    def msg(self, g, t, p, n):
        c, opp, fwd, back, stride = self.geom(t, p)
        direct = self.direct(g, p)
        part = (opp, back, fwd)[n]
        to = part if direct else (fwd, back, fwd)[n]
        to = self.d + (to - c) * stride
        size = SIZES[p]
        return pltpu.make_async_remote_copy(
            src_ref=self.bufs[p].at[t, pl.ds(part * size, size)], dst_ref=self.recvs[p].at[t, n],
            send_sem=self.send_sem.at[g], recv_sem=self.recv_sem.at[g, p, 0 if n == 0 and not direct else 1],
            device_id={'data': to}, device_id_type=MESH)

    def arrived(self, g, p, lo, hi):
        first, last = GROUPS[g]
        ref = self.recvs[p].at[pl.ds(first, last - first), pl.ds(lo, hi - lo)]
        pltpu.make_async_copy(ref, ref, self.recv_sem.at[g, p, 0 if hi == 1 else 1]).wait()

    def tiles(self, g, f):
        lo, hi = GROUPS[g]
        loop(hi, f, lo)

    def start(self, g):
        for n in range(2):
            self.tiles(g, lambda t: self.msg(g, t, 0, n).start())

    def chunks(self, p, f):
        step = min(SIZES[p], 4)
        if SIZES[p] == step:
            f(0, step)
        else:
            loop(SIZES[p] // step, lambda i: f(i * step, step))

    def middle(self, g, p):
        buf, rcv, size = self.bufs[p], self.recvs[p], SIZES[p]

        def one(t):
            fwd = self.geom(t, p)[2]

            def add(i, w):
                at = pl.ds(fwd * size + i, w)
                buf[t, at] = (buf[t, at].astype(F32) + rcv[t, 0, pl.ds(i, w)].astype(F32)).astype(BF16)
            self.chunks(p, add)
            self.msg(g, t, p, 2).start()
        self.arrived(g, p, 0, 1)
        self.tiles(g, one)

    def finish(self, g, p):
        buf, rcv, size = self.bufs[p], self.recvs[p], SIZES[p]
        first = 0 if self.direct(g, p) else 1

        def total(t, i, w):
            c = self.geom(t, p)[0]
            v = buf[t, pl.ds(c * size + i, w)].astype(F32)
            for n in range(first, 3):
                v = v + rcv[t, n, pl.ds(i, w)].astype(F32)
            return v

        def one(t):
            if p == 2:
                self.store(t, total(t, 0, 1)[0])
                return

            def put(i, w):
                self.bufs[p + 1][t, pl.ds(i, w)] = total(t, i, w).astype(BF16)
            self.chunks(p, put)
            self.msg(g, t, p + 1, 0).start()
        self.arrived(g, p, first, 3)
        if p == 2:
            for t in range(*GROUPS[g]):
                one(t)
            return
        self.tiles(g, one)
        for n in range(1, 3 if self.direct(g, p + 1) else 2):
            self.tiles(g, lambda t: self.msg(g, t, p + 1, n).start())

    def drain(self):
        for g, (first, last) in enumerate(GROUPS):
            ref = self.bufs[0].at[pl.ds(first, last - first), pl.ds(0, 63)]
            pltpu.make_async_copy(ref, ref, self.send_sem.at[g]).wait()


def layer_kernel(x_hbm, dy_hbm, wq_hbm, wk_hbm, wv_hbm, wo_hbm, dx_hbm, dwq_hbm, dwk_hbm, dwv_hbm, dwo_hbm,
                 x, dy, wq_raw, wq, wkv, wo, q, do, kv, kvt, ot, dqt, dq, dkv, dkv_in, dkvb, dx_in,
                 dwq_out, dwk_out, dwv_out, dwo_out, b0, b1, b2, r0, r1, r2, load_sem, pair_send, pair_recv, send_sem, recv_sem):
    m = lax.axis_index('model')

    def store(t, v):
        if t >= 16:
            out = (dwk_out, dwv_out)[t - 16]
            out[:, 0:128] = v[0:16]
            out[:, 128:256] = v[16:32]
        else:
            h, u = divmod(t, 4)
            cols = slice((u % 2) * 128, (u % 2) * 128 + 128)
            if u < 2:
                dwo_out[h, :, cols] = v
            else:
                dwq_out[:, h, cols] = v
    ring = Ring((b0, b1, b2), (r0, r1, r2), send_sem, recv_sem, store)
    own = block(m, HALF)
    away = block(1 - m, HALF)

    def load(src, dst, i):
        return pltpu.make_async_copy(src, dst, load_sem.at[i])

    def push(src, dst, i):
        return pltpu.make_async_remote_copy(src_ref=src, dst_ref=dst, send_sem=pair_send.at[i], recv_sem=pair_recv.at[i],
                                            device_id={'model': 1 - m}, device_id_type=MESH)
    loads = [load(x_hbm, x.at[own], 0), load(wq_hbm, wq_raw, 1), load(wk_hbm, wkv.at[:, 0:E], 2), load(wv_hbm, wkv.at[:, E:2 * E], 3),
             load(dy_hbm, dy.at[own], 4), load(wo_hbm, wo, 5)]
    for i in (1, 0, 2, 3, 4, 5):
        loads[i].start()
    sem = pltpu.get_barrier_semaphore()
    ring.greet(sem)
    pl.semaphore_signal(sem, inc=1, device_id={'model': 1 - m}, device_id_type=MESH)
    dkv[...] = jnp.zeros_like(dkv)
    loads[1].wait()

    def flatten(i):
        rows = block(i, 128)
        wq[rows] = wq_raw[rows].reshape(128, NH * E)
    loop(16, flatten)
    pl.semaphore_wait(sem, 10)
    push_x = push(x_hbm, x.at[own], 0)
    push_dy = push(dy_hbm, dy.at[own], 1)
    push_x.start()
    push_dy.start()

    def project_q(h, rows):
        q[h, rows] = nn(x[rows], wq[:, block(h, E)]).astype(BF16)

    def project_do(h, rows):
        do[h, rows] = nt(dy[rows], wo[block(h, E)]).astype(BF16)

    def project_kv(rows):
        kv[rows] = nn(x[rows], wkv[...]).astype(BF16)

    def project_q_own(i):
        for h in range(2):
            project_q(i * 2 + h, own)

    def project_do_own(i):
        for h in range(2):
            project_do(i * 2 + h, own)
    for i in (0, 2, 3):
        loads[i].wait()
    loop(2, project_q_own)
    project_kv(own)
    loads[4].wait()
    loads[5].wait()
    loop(2, project_do_own)
    push_x.wait_recv()
    project_kv(away)
    project_q(0, away)
    push_dy.wait_recv()
    project_do(0, away)

    def turn(i):
        cols = block(i, 256)
        kvt[0:E, cols] = kv[cols, 0:E].T
        kvt[E:2 * E, cols] = kv[cols, E:2 * E].T
    loop(4, turn)

    def attend(h, j):
        n = (j + 1) * 256
        rows = slice(j * 256, n)
        qb = q[h, rows]
        dob = do[h, rows]
        st = nt(kv[0:n, 0:E], qb)
        dpt = nt(kv[0:n, E:2 * E], dob)
        yield
        keep = lax.broadcasted_iota(jnp.int32, (256, 256), 0) <= lax.broadcasted_iota(jnp.int32, (256, 256), 1)
        diag = jnp.where(keep, st[n - 256:n], -jnp.inf)
        st = diag if j == 0 else jnp.concatenate([st[0:n - 256], diag], axis=0)
        top = jnp.max(st, axis=0, keepdims=True)
        pt = jnp.exp2((st - top) * (CD * LOG2E))
        pt = pt * (1.0 / jnp.sum(pt, axis=0, keepdims=True))
        pb = pt.astype(BF16)
        yield
        ob = nn(kvt[E:2 * E, 0:n], pb).astype(BF16)
        ot[:, rows] = ob
        delta = jnp.sum(dob.T.astype(F32) * ob.astype(F32), axis=0, keepdims=True)
        dkv[0:n, E:2 * E] += nn(pb, dob)
        yield
        dst = (pt * (dpt - delta)).astype(BF16)
        yield
        dqb = (nn(kvt[0:E, 0:n], dst) * CD).astype(BF16)
        dqt[:, rows] = dqb
        dq[rows, block(h, E)] = dqb.T
        dkv[0:n, 0:E] += nn(dst, qb)
        yield

    def attention(h):
        todo = [attend(h, j) for j in (3, 2, 1, 0)]
        for tick in range(5 + 2 * 3):
            for b, stages in enumerate(todo):
                if 0 <= tick - 2 * b < 5:
                    next(stages)
            if tick == 1:
                project_q((h + 1) % NH, away)
            if tick == 5:
                project_do((h + 1) % NH, away)

    def store_tiles(t, v, i):
        sx, sy, sz = steps_of(t)
        base = (i % 2) * 2 * sy + (i // 2) * sz
        for j in range(8):
            at = base + (j % 4) * sx + (j // 4) * sy
            for u in range(2):
                b0[t + u, at] = v[j * 32:(j + 1) * 32, u * 128:(u + 1) * 128]

    def weight_grads(h, i):
        vo = nn(ot[...], dy[:, block(i, 512)]).astype(BF16).T
        vq = nn(dqt[...], x[:, block(i, 512)]).astype(BF16).T
        for u in range(2):
            store_tiles(h * 4, vo[u * 256:(u + 1) * 256], i * 2 + u)
            store_tiles(h * 4 + 2, vq[u * 256:(u + 1) * 256], i * 2 + u)
    push_kv = push(dkv, dkv_in, 2)

    def head_step(h):
        attention(h)

        @pl.when(h == NH - 1)
        def _():
            push_kv.start()
            ring.middle(0, 1)

        def grads_step(i):
            weight_grads(h, i)

            def at(hh, ii, f):
                @pl.when((h == hh) & (i == ii))
                def _():
                    f()
            for hh in range(2, NH):
                at(hh, 0, lambda: ring.finish(hh - 2, 0))
            for hh in range(1, NH):
                at(hh, 2, lambda: ring.middle(hh - 1, 0))
            for hh in range(NH):
                at(hh, 3, lambda: ring.start(hh))
        loop(4, grads_step)
    loop(NH, head_step)
    ring.finish(0, 1)
    ring.middle(1, 1)

    push_kv.wait_recv()

    def kv_sum(i):
        rows = block(i, 128)
        v = dkv[rows] + dkv_in[rows]
        dkvb[rows, 0:E] = (v[:, 0:E] * CD).astype(BF16)
        dkvb[rows, E:2 * E] = v[:, E:2 * E].astype(BF16)
    loop(8, kv_sum)

    def kv_block(i):
        v = tn(x[:, block(m * 4 + i, 256)], dkvb[...]).astype(BF16)
        for j in range(16):
            rows = v[j * 16:(j + 1) * 16]
            at = i * 16 + (j % 4) * 4 + j // 4
            for u in range(2):
                b0[16 + u, at, 0:16] = rows[:, u * E:u * E + 128]
                b0[16 + u, at, 16:32] = rows[:, u * E + 128:u * E + 256]
    loop(4, kv_block)
    ring.start(4)

    def dx_away(i):
        cols = block(i, 512)
        wo[0:HALF, cols] = nt(dq[away], wq[cols]).astype(BF16)
    def push_dx(i):
        cols = pl.ds(i * 1024, 1024)
        return push(wo.at[pl.ds(0, HALF), cols], dx_in.at[:, cols], 3 + i)
    loop(2, dx_away)
    push_dx(0).start()
    ring.middle(3, 0)
    ring.finish(2, 0)
    loop(4, dx_away, 2)
    push_dx(1).start()
    ring.middle(4, 0)
    ring.finish(1, 1)
    ring.finish(0, 2)

    def dx_own(i):
        cols = block(i, 512)
        v = nt(dq[own], wq[cols]) + nt(dkvb[own], wkv[cols])
        wo[HALF:SEQ, cols] = (v + dx_in[:, cols].astype(F32)).astype(BF16)
    push_dx(0).wait_recv()
    loop(1, dx_own)
    ring.middle(2, 1)
    ring.finish(3, 0)
    loop(2, dx_own, 1)
    ring.finish(4, 0)
    push_dx(1).wait_recv()
    loop(3, dx_own, 2)
    ring.finish(2, 1)
    ring.finish(1, 2)
    loop(4, dx_own, 3)
    store_dx = load(wo.at[pl.ds(HALF, HALF)], dx_hbm, 6)
    store_dx.start()
    ring.finish(3, 1)
    ring.finish(4, 1)
    for g in (2, 3, 4):
        ring.finish(g, 2)
    stores = [load(a, b, 7 + i) for i, (a, b) in enumerate(
        ((dwq_out, dwq_hbm), (dwk_out, dwk_hbm), (dwv_out, dwv_hbm), (dwo_out, dwo_hbm)))]
    for c in stores:
        c.start()
    ring.drain()
    for c in stores:
        c.wait()
    for c in (push_x, push_dy, push_kv, push_dx(0), push_dx(1)):
        c.wait_send()
    store_dx.wait()


def layer(x, dy, wq, wk, wv, wo):
    hbm = pl.BlockSpec(memory_space=pl.ANY)
    dma = pltpu.SemaphoreType.DMA
    bf = lambda *shape: pltpu.VMEM(shape, BF16)
    return pl.pallas_call(
        layer_kernel,
        out_shape=(jax.ShapeDtypeStruct((HALF, D), BF16), jax.ShapeDtypeStruct((32, NH, E), F32),
                   jax.ShapeDtypeStruct((16, E), F32), jax.ShapeDtypeStruct((16, E), F32), jax.ShapeDtypeStruct((NH, 32, E), F32)),
        in_specs=[hbm] * 6, out_specs=[hbm] * 5,
        scratch_shapes=[
            bf(SEQ, D), bf(SEQ, D), bf(D, NH, E), bf(D, NH * E), bf(D, 2 * E), bf(NH * E, D),
            bf(NH, SEQ, E), bf(NH, SEQ, E), bf(SEQ, 2 * E), bf(2 * E, SEQ), bf(E, SEQ), bf(E, SEQ), bf(SEQ, NH * E),
            pltpu.VMEM((SEQ, 2 * E), F32), pltpu.VMEM((SEQ, 2 * E), F32), bf(SEQ, 2 * E), bf(HALF, D),
            pltpu.VMEM((32, NH, E), F32), pltpu.VMEM((16, E), F32), pltpu.VMEM((16, E), F32), pltpu.VMEM((NH, 32, E), F32),
            bf(NT, 64, 32, 128), bf(NT, 16, 32, 128), bf(NT, 4, 32, 128),
            bf(NT, 3, 16, 32, 128), bf(NT, 3, 4, 32, 128), bf(NT, 3, 1, 32, 128),
            dma((11,)), dma((5,)), dma((5,)), dma((len(GROUPS),)), dma((len(GROUPS), 3, 2))],
        compiler_params=pltpu.CompilerParams(collective_id=0, has_side_effects=True, vmem_limit_bytes=67043328),
        cost_estimate=pl.CostEstimate(flops=3 * 10 ** 10, bytes_accessed=2 * 10 ** 7, transcendentals=0),
    )(x, dy, wq, wk, wv, wo)


def hand_on_kernel(dx, dwq, dwk, dwv, dwo, dx_out, dwq_out, dwk_out, dwv_out, dwo_out, dx_v, dwq_v, dwk_v, dwv_v, dwo_v, sem_in, sem_out):
    pieces = [(dx.at[pl.ds(i * 128, 128)], dx_v.at[pl.ds(i * 128, 128)], dx_out.at[pl.ds(i * 128, 128)]) for i in range(4)]
    pieces += [(dwq, dwq_v, dwq_out), (dwk, dwk_v, dwk_out), (dwv, dwv_v, dwv_out), (dwo, dwo_v, dwo_out)]
    reads = [pltpu.make_async_copy(a, b, sem_in.at[i]) for i, (a, b, _) in enumerate(pieces)]
    writes = [pltpu.make_async_copy(b, c, sem_out.at[i]) for i, (_, b, c) in enumerate(pieces)]
    for c in reads:
        c.start()
    for r, w in zip(reads, writes):
        r.wait()
        w.start()
    for w in writes:
        w.wait()


def hand_on(*arrays):
    hbm = pl.BlockSpec(memory_space=pl.ANY)
    return pl.pallas_call(
        hand_on_kernel,
        out_shape=tuple(jax.ShapeDtypeStruct(a.shape, a.dtype) for a in arrays),
        in_specs=[hbm] * 5, out_specs=[hbm] * 5,
        scratch_shapes=[pltpu.VMEM(a.shape, a.dtype) for a in arrays] + [pltpu.SemaphoreType.DMA((8,)), pltpu.SemaphoreType.DMA((8,))],
        cost_estimate=pl.CostEstimate(flops=10 ** 6, bytes_accessed=6 * 10 ** 6, transcendentals=0),
    )(*arrays)


def solution(mesh):
    tok_spec = P(('pod', 'data'), 'model', None)

    def device_step(x_loc, dy_loc, w_q, w_k, w_v, w_o):
        dx, dwq, dwk, dwv, dwo = hand_on(*layer(x_loc[0], dy_loc[0], w_q, w_k[0], w_v[0], w_o.reshape(NH * E, D)))
        return dx[None], dwq, dwk, dwv, dwo.transpose(0, 2, 1)

    kv_rows = P(('pod', 'model', 'data'), None)
    return jax.shard_map(device_step, mesh=mesh,
                         in_specs=(tok_spec, tok_spec, P(None, 'model', None), P(), P(), P('model', None, None)),
                         out_specs=(tok_spec, P(('pod', 'data'), 'model', None), kv_rows, kv_rows, P(('pod', 'model'), None, 'data')),
                         check_vma=False)
```

```python
import jax
import jax.numpy as jnp
from jax import lax
from jax.experimental import pallas as pl
from jax.experimental.pallas import tpu as pltpu
from jax.sharding import PartitionSpec as P

MESH = pl.DeviceIdType.MESH
BF16 = jnp.bfloat16
F32 = jnp.float32
NT = 18
SIZES = (16, 4, 1)
GROUPS = ((0, 4), (4, 8), (8, 12), (12, 16), (16, 18))
SEQ, HALF, D, E, NH = 1024, 512, 2048, 256, 4
CD = E ** -0.5
LOG2E = 1.4426950408889634


def nn(a, b):
    return lax.dot_general(a, b, (((1,), (0,)), ((), ())), preferred_element_type=F32)


def nt(a, b):
    return lax.dot_general(a, b, (((1,), (1,)), ((), ())), preferred_element_type=F32)


def tn(a, b):
    return lax.dot_general(a, b, (((0,), (0,)), ((), ())), preferred_element_type=F32)


def loop(n, f, start=0):
    def body(i, _):
        f(i)
        return 0
    lax.fori_loop(start, n, body, 0)


def block(i, size):
    return pl.ds(pl.multiple_of(i * size, size), size)


def pick(i, a, b, c):
    return a * ((1 - i) * (2 - i) // 2) + b * (i * (2 - i)) + c * (i * (i - 1) // 2)


def steps_of(t):
    k = (t // 2) % 3
    return pick(k, 16, 1, 4), pick(k, 4, 16, 1), pick(k, 1, 4, 16)


class Ring:
    def __init__(self, bufs, recvs, send_sem, recv_sem, store):
        self.bufs, self.recvs, self.send_sem, self.recv_sem, self.store = bufs, recvs, send_sem, recv_sem, store
        d = lax.axis_index('data')
        coords = (d % 4, (d // 4) % 4, d // 16)
        self.at = [[((c + k) % 4, d + ((c + k) % 4 - c) * 4 ** ax) for k in range(4)] for ax, c in enumerate(coords)]

    def greet(self, sem):
        for ax in range(3):
            for k in (1, 3, 2):
                pl.semaphore_signal(sem, inc=1, device_id={'data': self.at[ax][k][1]}, device_id_type=MESH)

    def ways(self, t, p):
        ring = self.at[((t // 2) % 3 + p) % 3]
        return (ring[0], ring[2], ring[1], ring[3]) if t % 2 == 0 else (ring[0], ring[2], ring[3], ring[1])

    def direct(self, g, p):
        return p == 2 or (p == 1 and g >= 3)

    def msg(self, g, t, p, n):
        _, opp, fwd, back = self.ways(t, p)
        direct = self.direct(g, p)
        part = (opp, back, fwd)[n]
        to = part if direct else (fwd, back, fwd)[n]
        size = SIZES[p]
        return pltpu.make_async_remote_copy(
            src_ref=self.bufs[p].at[t, pl.ds(part[0] * size, size)], dst_ref=self.recvs[p].at[t, n],
            send_sem=self.send_sem.at[g], recv_sem=self.recv_sem.at[g, p, 0 if n == 0 and not direct else 1],
            device_id={'data': to[1]}, device_id_type=MESH)

    def arrived(self, g, p, lo, hi):
        first, last = GROUPS[g]
        ref = self.recvs[p].at[pl.ds(first, last - first), pl.ds(lo, hi - lo)]
        pltpu.make_async_copy(ref, ref, self.recv_sem.at[g, p, 0 if hi == 1 else 1]).wait()

    def tiles(self, g, f):
        for t in range(*GROUPS[g]):
            f(t)

    def start(self, g):
        for n in range(2):
            self.tiles(g, lambda t: self.msg(g, t, 0, n).start())

    def chunks(self, p, f):
        step = min(SIZES[p], 8)
        for i in range(0, SIZES[p], step):
            f(i, step)

    def middle(self, g, p):
        buf, rcv, size = self.bufs[p], self.recvs[p], SIZES[p]

        def one(t):
            fwd = self.ways(t, p)[2][0]

            def add(i, w):
                at = pl.ds(fwd * size + i, w)
                buf[t, at] = (buf[t, at].astype(F32) + rcv[t, 0, pl.ds(i, w)].astype(F32)).astype(BF16)
            self.chunks(p, add)
            self.msg(g, t, p, 2).start()
        self.arrived(g, p, 0, 1)
        self.tiles(g, one)

    def finish(self, g, p):
        buf, rcv, size = self.bufs[p], self.recvs[p], SIZES[p]
        first = 0 if self.direct(g, p) else 1

        def total(t, i, w):
            c = self.ways(t, p)[0][0]
            v = buf[t, pl.ds(c * size + i, w)].astype(F32)
            for n in range(first, 3):
                v = v + rcv[t, n, pl.ds(i, w)].astype(F32)
            return v

        def one(t):
            if p == 2:
                self.store(t, total(t, 0, 1)[0])
                return

            def put(i, w):
                self.bufs[p + 1][t, pl.ds(i, w)] = total(t, i, w).astype(BF16)
            self.chunks(p, put)
            self.msg(g, t, p + 1, 0).start()
        self.arrived(g, p, first, 3)
        self.tiles(g, one)
        if p < 2:
            for n in range(1, 3 if self.direct(g, p + 1) else 2):
                self.tiles(g, lambda t: self.msg(g, t, p + 1, n).start())

    def drain(self):
        for g, (first, last) in enumerate(GROUPS):
            ref = self.bufs[0].at[pl.ds(first, last - first), pl.ds(0, 63)]
            pltpu.make_async_copy(ref, ref, self.send_sem.at[g]).wait()


def layer_kernel(x_hbm, dy_hbm, wq_hbm, wk_hbm, wv_hbm, wo_hbm, dx_hbm, dwq_hbm, dwk_hbm, dwv_hbm, dwo_hbm,
                 x, dy, wq_raw, wq, wkv, wo, q, do, kv, kvt, ot, dqt, dq, dkv, dkv_in, dkvb, dx_in,
                 dwq_out, dwk_out, dwv_out, dwo_out, b0, b1, b2, r0, r1, r2, load_sem, pair_send, pair_recv, send_sem, recv_sem):
    m = lax.axis_index('model')

    def store(t, v):
        if t >= 16:
            out = (dwk_out, dwv_out)[t - 16]
            out[:, 0:128] = v[0:16]
            out[:, 128:256] = v[16:32]
        else:
            h, u = divmod(t, 4)
            cols = slice((u % 2) * 128, (u % 2) * 128 + 128)
            if u < 2:
                dwo_out[h, :, cols] = v
            else:
                dwq_out[:, h, cols] = v
    ring = Ring((b0, b1, b2), (r0, r1, r2), send_sem, recv_sem, store)
    own = block(m, HALF)
    away = block(1 - m, HALF)

    def load(src, dst, i):
        return pltpu.make_async_copy(src, dst, load_sem.at[i])

    def push(src, dst, i):
        return pltpu.make_async_remote_copy(src_ref=src, dst_ref=dst, send_sem=pair_send.at[i], recv_sem=pair_recv.at[i],
                                            device_id={'model': 1 - m}, device_id_type=MESH)
    loads = [load(x_hbm, x.at[own], 0), load(wq_hbm, wq_raw, 1), load(wk_hbm, wkv.at[:, 0:E], 2), load(wv_hbm, wkv.at[:, E:2 * E], 3),
             load(dy_hbm, dy.at[own], 4), load(wo_hbm, wo, 5)]
    for i in (0, 2, 3, 1, 4, 5):
        loads[i].start()
    sem = pltpu.get_barrier_semaphore()
    ring.greet(sem)
    pl.semaphore_signal(sem, inc=1, device_id={'model': 1 - m}, device_id_type=MESH)
    dkv[...] = jnp.zeros_like(dkv)

    def project_q(h, rows):
        q[h, rows] = nn(x[rows], wq[:, block(h, E)]).astype(BF16)

    def project_do(h, rows):
        do[h, rows] = nt(dy[rows], wo[block(h, E)]).astype(BF16)

    def project_q_own(i):
        for h in range(2):
            project_q(i * 2 + h, own)

    def project_do_own(i):
        for h in range(2):
            project_do(i * 2 + h, own)

    def flatten(i):
        rows = block(i, 128)
        wq[rows] = wq_raw[rows].reshape(128, NH * E)

    def turn(i):
        cols = block(i, 256)
        kvt[0:E, cols] = kv[cols, 0:E].T
        kvt[E:2 * E, cols] = kv[cols, E:2 * E].T
    for i in (0, 2, 3):
        loads[i].wait()
    kv[own] = nn(x[own], wkv[...]).astype(BF16)
    pl.semaphore_wait(sem, 10)
    push_k = push(kv.at[own], kv.at[own], 5)
    push_x = push(x_hbm, x.at[own], 0)
    push_dy = push(dy_hbm, dy.at[own], 1)
    push_k.start()
    push_x.start()
    push_dy.start()
    loads[1].wait()
    loop(16, flatten)
    loop(2, project_q_own)
    loads[4].wait()
    loads[5].wait()
    loop(2, project_do_own)
    push_k.wait_recv()
    loop(4, turn)
    push_x.wait_recv()
    project_q(0, away)
    push_dy.wait_recv()
    project_do(0, away)

    def attend(h, j):
        n = (j + 1) * 256
        rows = slice(j * 256, n)
        qb = q[h, rows]
        dob = do[h, rows]
        st = nt(kv[0:n, 0:E], qb)
        dpt = nt(kv[0:n, E:2 * E], dob)
        yield
        keep = lax.broadcasted_iota(jnp.int32, (256, 256), 0) <= lax.broadcasted_iota(jnp.int32, (256, 256), 1)
        diag = jnp.where(keep, st[n - 256:n], -jnp.inf)
        st = diag if j == 0 else jnp.concatenate([st[0:n - 256], diag], axis=0)
        top = jnp.max(st, axis=0, keepdims=True)
        pt = jnp.exp2((st - top) * (CD * LOG2E))
        pt = pt * (1.0 / jnp.sum(pt, axis=0, keepdims=True))
        pb = pt.astype(BF16)
        yield
        ob = nn(kvt[E:2 * E, 0:n], pb).astype(BF16)
        ot[:, rows] = ob
        delta = jnp.sum(dob.T.astype(F32) * ob.astype(F32), axis=0, keepdims=True)
        dkv[0:n, E:2 * E] += nn(pb, dob)
        yield
        dst = (pt * (dpt - delta)).astype(BF16)
        yield
        dqb = (nn(kvt[0:E, 0:n], dst) * CD).astype(BF16)
        dqt[:, rows] = dqb
        dq[rows, block(h, E)] = dqb.T
        dkv[0:n, 0:E] += nn(dst, qb)
        yield

    def attention(h):
        todo = [attend(h, j) for j in (3, 2, 1, 0)]
        for tick in range(5 + 2 * 3):
            for b, stages in enumerate(todo):
                if 0 <= tick - 2 * b < 5:
                    next(stages)
            if tick == 1:
                project_q((h + 1) % NH, away)
            if tick == 5:
                project_do((h + 1) % NH, away)

    def store_tiles(t, v, i):
        sx, sy, sz = steps_of(t)
        base = (i % 2) * 2 * sy + (i // 2) * sz
        for j in range(8):
            at = base + (j % 4) * sx + (j // 4) * sy
            for u in range(2):
                b0[t + u, at] = v[j * 32:(j + 1) * 32, u * 128:(u + 1) * 128]

    def weight_grads(h, i):
        vo = nn(ot[...], dy[:, block(i, 512)]).astype(BF16).T
        vq = nn(dqt[...], x[:, block(i, 512)]).astype(BF16).T
        for u in range(2):
            store_tiles(h * 4, vo[u * 256:(u + 1) * 256], i * 2 + u)
            store_tiles(h * 4 + 2, vq[u * 256:(u + 1) * 256], i * 2 + u)
    push_kv = push(dkv, dkv_in, 2)

    def head_step(h):
        attention(h)

        @pl.when(h == NH - 1)
        def _():
            push_kv.start()
            ring.middle(0, 1)

        def grads_step(i):
            weight_grads(h, i)

            def at(hh, ii, f):
                @pl.when((h == hh) & (i == ii))
                def _():
                    f()
            for hh in range(2, NH):
                at(hh, 0, lambda: ring.finish(hh - 2, 0))
            for hh in range(1, NH):
                at(hh, 2, lambda: ring.middle(hh - 1, 0))
            for hh in range(NH):
                at(hh, 3, lambda: ring.start(hh))
        loop(4, grads_step)
    loop(NH, head_step)
    ring.finish(0, 1)
    ring.middle(1, 1)

    push_kv.wait_recv()

    def kv_sum(i):
        rows = block(i, 128)
        v = dkv[rows] + dkv_in[rows]
        dkvb[rows, 0:E] = (v[:, 0:E] * CD).astype(BF16)
        dkvb[rows, E:2 * E] = v[:, E:2 * E].astype(BF16)
    loop(8, kv_sum)

    def kv_block(i):
        v = tn(x[:, block(m * 4 + i, 256)], dkvb[...]).astype(BF16)
        for j in range(16):
            rows = v[j * 16:(j + 1) * 16]
            at = i * 16 + (j % 4) * 4 + j // 4
            for u in range(2):
                b0[16 + u, at, 0:16] = rows[:, u * E:u * E + 128]
                b0[16 + u, at, 16:32] = rows[:, u * E + 128:u * E + 256]
    loop(4, kv_block)
    ring.start(4)

    def dx_away(i):
        cols = block(i, 512)
        wo[0:HALF, cols] = nt(dq[away], wq[cols]).astype(BF16)
    def push_dx(i):
        cols = pl.ds(i * 1024, 1024)
        return push(wo.at[pl.ds(0, HALF), cols], dx_in.at[:, cols], 3 + i)
    loop(2, dx_away)
    push_dx(0).start()
    ring.middle(3, 0)
    ring.finish(2, 0)
    loop(4, dx_away, 2)
    push_dx(1).start()
    ring.middle(4, 0)
    ring.finish(1, 1)
    ring.finish(0, 2)

    def dx_own(i):
        cols = block(i, 512)
        v = nt(dq[own], wq[cols]) + nt(dkvb[own], wkv[cols])
        wo[HALF:SEQ, cols] = (v + dx_in[:, cols].astype(F32)).astype(BF16)
    push_dx(0).wait_recv()
    loop(1, dx_own)
    ring.middle(2, 1)
    ring.finish(3, 0)
    loop(2, dx_own, 1)
    ring.finish(4, 0)
    push_dx(1).wait_recv()
    loop(3, dx_own, 2)
    ring.finish(2, 1)
    ring.finish(1, 2)
    loop(4, dx_own, 3)
    store_dx = load(wo.at[pl.ds(HALF, HALF)], dx_hbm, 6)
    store_dx.start()
    ring.finish(3, 1)
    ring.finish(4, 1)
    for g in (2, 3, 4):
        ring.finish(g, 2)
    stores = [load(a, b, 7 + i) for i, (a, b) in enumerate(
        ((dwq_out, dwq_hbm), (dwk_out, dwk_hbm), (dwv_out, dwv_hbm), (dwo_out, dwo_hbm)))]
    for c in stores:
        c.start()
    ring.drain()
    for c in stores:
        c.wait()
    for c in (push_k, push_x, push_dy, push_kv, push_dx(0), push_dx(1)):
        c.wait_send()
    store_dx.wait()


def layer(x, dy, wq, wk, wv, wo):
    hbm = pl.BlockSpec(memory_space=pl.ANY)
    dma = pltpu.SemaphoreType.DMA
    bf = lambda *shape: pltpu.VMEM(shape, BF16)
    return pl.pallas_call(
        layer_kernel,
        out_shape=(jax.ShapeDtypeStruct((HALF, D), BF16), jax.ShapeDtypeStruct((32, NH, E), F32),
                   jax.ShapeDtypeStruct((16, E), F32), jax.ShapeDtypeStruct((16, E), F32), jax.ShapeDtypeStruct((NH, 32, E), F32)),
        in_specs=[hbm] * 6, out_specs=[hbm] * 5,
        scratch_shapes=[
            bf(SEQ, D), bf(SEQ, D), bf(D, NH, E), bf(D, NH * E), bf(D, 2 * E), bf(NH * E, D),
            bf(NH, SEQ, E), bf(NH, SEQ, E), bf(SEQ, 2 * E), bf(2 * E, SEQ), bf(E, SEQ), bf(E, SEQ), bf(SEQ, NH * E),
            pltpu.VMEM((SEQ, 2 * E), F32), pltpu.VMEM((SEQ, 2 * E), F32), bf(SEQ, 2 * E), bf(HALF, D),
            pltpu.VMEM((32, NH, E), F32), pltpu.VMEM((16, E), F32), pltpu.VMEM((16, E), F32), pltpu.VMEM((NH, 32, E), F32),
            bf(NT, 64, 32, 128), bf(NT, 16, 32, 128), bf(NT, 4, 32, 128),
            bf(NT, 3, 16, 32, 128), bf(NT, 3, 4, 32, 128), bf(NT, 3, 1, 32, 128),
            dma((11,)), dma((6,)), dma((6,)), dma((len(GROUPS),)), dma((len(GROUPS), 3, 2))],
        compiler_params=pltpu.CompilerParams(collective_id=0, has_side_effects=True, vmem_limit_bytes=67043328),
        cost_estimate=pl.CostEstimate(flops=3 * 10 ** 10, bytes_accessed=2 * 10 ** 7, transcendentals=0),
    )(x, dy, wq, wk, wv, wo)


def hand_on_kernel(dx, dwq, dwk, dwv, dwo, dx_out, dwq_out, dwk_out, dwv_out, dwo_out, dx_v, dwq_v, dwk_v, dwv_v, dwo_v, sem_in, sem_out):
    pieces = [(dx.at[pl.ds(i * 128, 128)], dx_v.at[pl.ds(i * 128, 128)], dx_out.at[pl.ds(i * 128, 128)]) for i in range(4)]
    pieces += [(dwq, dwq_v, dwq_out), (dwk, dwk_v, dwk_out), (dwv, dwv_v, dwv_out), (dwo, dwo_v, dwo_out)]
    reads = [pltpu.make_async_copy(a, b, sem_in.at[i]) for i, (a, b, _) in enumerate(pieces)]
    writes = [pltpu.make_async_copy(b, c, sem_out.at[i]) for i, (_, b, c) in enumerate(pieces)]
    for c in reads:
        c.start()
    for r, w in zip(reads, writes):
        r.wait()
        w.start()
    for w in writes:
        w.wait()


def hand_on(*arrays):
    hbm = pl.BlockSpec(memory_space=pl.ANY)
    return pl.pallas_call(
        hand_on_kernel,
        out_shape=tuple(jax.ShapeDtypeStruct(a.shape, a.dtype) for a in arrays),
        in_specs=[hbm] * 5, out_specs=[hbm] * 5,
        scratch_shapes=[pltpu.VMEM(a.shape, a.dtype) for a in arrays] + [pltpu.SemaphoreType.DMA((8,)), pltpu.SemaphoreType.DMA((8,))],
        cost_estimate=pl.CostEstimate(flops=10 ** 6, bytes_accessed=6 * 10 ** 6, transcendentals=0),
    )(*arrays)


def solution(mesh):
    tok_spec = P(('pod', 'data'), 'model', None)

    def device_step(x_loc, dy_loc, w_q, w_k, w_v, w_o):
        dx, dwq, dwk, dwv, dwo = hand_on(*layer(x_loc[0], dy_loc[0], w_q, w_k[0], w_v[0], w_o.reshape(NH * E, D)))
        return dx[None], dwq, dwk, dwv, dwo.transpose(0, 2, 1)

    kv_rows = P(('pod', 'model', 'data'), None)
    return jax.shard_map(device_step, mesh=mesh,
                         in_specs=(tok_spec, tok_spec, P(None, 'model', None), P(), P(), P('model', None, None)),
                         out_specs=(tok_spec, P(('pod', 'data'), 'model', None), kv_rows, kv_rows, P(('pod', 'model'), None, 'data')),
                         check_vma=False)
```

```python
import jax
import jax.numpy as jnp
from jax import lax
from jax.experimental import pallas as pl
from jax.experimental.pallas import tpu as pltpu
from jax.sharding import PartitionSpec as P

MESH = pl.DeviceIdType.MESH
BF16 = jnp.bfloat16
F32 = jnp.float32
NT = 18
SIZES = (16, 4, 1)
GROUPS = ((0, 4), (4, 8), (8, 12), (12, 14), (14, 16), (16, 18))
COLOURS = (0, 1, 2, 0, 1, 2, 1, 0, 2)
SEQ, HALF, D, E, NH = 1024, 512, 2048, 256, 4
CD = E ** -0.5
LOG2E = 1.4426950408889634


def nn(a, b):
    return lax.dot_general(a, b, (((1,), (0,)), ((), ())), preferred_element_type=F32)


def nt(a, b):
    return lax.dot_general(a, b, (((1,), (1,)), ((), ())), preferred_element_type=F32)


def tn(a, b):
    return lax.dot_general(a, b, (((0,), (0,)), ((), ())), preferred_element_type=F32)


def loop(n, f, start=0):
    def body(i, _):
        f(i)
        return 0
    lax.fori_loop(start, n, body, 0)


def block(i, size):
    return pl.ds(pl.multiple_of(i * size, size), size)


def steps_of(t):
    return ((16, 4, 1), (1, 16, 4), (4, 1, 16))[COLOURS[t // 2]]


class Ring:
    def __init__(self, bufs, recvs, send_sem, recv_sem, store):
        self.bufs, self.recvs, self.send_sem, self.recv_sem, self.store = bufs, recvs, send_sem, recv_sem, store
        d = lax.axis_index('data')
        coords = (d % 4, (d // 4) % 4, d // 16)
        self.at = [[((c + k) % 4, d + ((c + k) % 4 - c) * 4 ** ax) for k in range(4)] for ax, c in enumerate(coords)]

    def greet(self, sem):
        for ax in range(3):
            for k in (1, 3, 2):
                pl.semaphore_signal(sem, inc=1, device_id={'data': self.at[ax][k][1]}, device_id_type=MESH)

    def ways(self, t, p):
        ring = self.at[(COLOURS[t // 2] + p) % 3]
        return (ring[0], ring[2], ring[1], ring[3]) if t % 2 == 0 else (ring[0], ring[2], ring[3], ring[1])

    def direct(self, g, p):
        return p == 2 or (p == 1 and g >= 2)

    def msg(self, g, t, p, n):
        _, opp, fwd, back = self.ways(t, p)
        direct = self.direct(g, p)
        part = (opp, back, fwd)[n]
        to = part if direct else (fwd, back, fwd)[n]
        size = SIZES[p]
        return pltpu.make_async_remote_copy(
            src_ref=self.bufs[p].at[t, pl.ds(part[0] * size, size)], dst_ref=self.recvs[p].at[t, n],
            send_sem=self.send_sem.at[g], recv_sem=self.recv_sem.at[g, p, 0 if n == 0 and not direct else 1],
            device_id={'data': to[1]}, device_id_type=MESH)

    def arrived(self, g, p, lo, hi):
        first, last = GROUPS[g]
        ref = self.recvs[p].at[pl.ds(first, last - first), pl.ds(lo, hi - lo)]
        pltpu.make_async_copy(ref, ref, self.recv_sem.at[g, p, 0 if hi == 1 else 1]).wait()

    def tiles(self, g, f):
        for t in range(*GROUPS[g]):
            f(t)

    def start(self, g):
        for n in range(2):
            self.tiles(g, lambda t: self.msg(g, t, 0, n).start())

    def chunks(self, p, f):
        step = min(SIZES[p], 8)
        for i in range(0, SIZES[p], step):
            f(i, step)

    def middle(self, g, p):
        buf, rcv, size = self.bufs[p], self.recvs[p], SIZES[p]

        def one(t):
            fwd = self.ways(t, p)[2][0]

            def add(i, w):
                at = pl.ds(fwd * size + i, w)
                buf[t, at] = (buf[t, at].astype(F32) + rcv[t, 0, pl.ds(i, w)].astype(F32)).astype(BF16)
            self.chunks(p, add)
            self.msg(g, t, p, 2).start()
        self.arrived(g, p, 0, 1)
        self.tiles(g, one)

    def finish(self, g, p):
        buf, rcv, size = self.bufs[p], self.recvs[p], SIZES[p]
        first = 0 if self.direct(g, p) else 1

        def total(t, i, w):
            c = self.ways(t, p)[0][0]
            v = buf[t, pl.ds(c * size + i, w)].astype(F32)
            for n in range(first, 3):
                v = v + rcv[t, n, pl.ds(i, w)].astype(F32)
            return v

        def one(t):
            if p == 2:
                self.store(t, total(t, 0, 1)[0])
                return

            def put(i, w):
                self.bufs[p + 1][t, pl.ds(i, w)] = total(t, i, w).astype(BF16)
            self.chunks(p, put)
            self.msg(g, t, p + 1, 0).start()
        self.arrived(g, p, first, 3)
        self.tiles(g, one)
        if p < 2:
            for n in range(1, 3 if self.direct(g, p + 1) else 2):
                self.tiles(g, lambda t: self.msg(g, t, p + 1, n).start())

    def drain(self):
        for g, (first, last) in enumerate(GROUPS):
            ref = self.bufs[0].at[pl.ds(first, last - first), pl.ds(0, 63)]
            pltpu.make_async_copy(ref, ref, self.send_sem.at[g]).wait()


def layer_kernel(x_hbm, dy_hbm, wq_hbm, wk_hbm, wv_hbm, wo_hbm, dx_hbm, dwq_hbm, dwk_hbm, dwv_hbm, dwo_hbm,
                 x, dy, wq_raw, wq, wkv, wo, q, do, kv, kvt, ot, dqt, dq, dkv, dkv_in, dkvb, dx_in,
                 dwq_out, dwk_out, dwv_out, dwo_out, b0, b1, b2, r0, r1, r2, load_sem, pair_send, pair_recv, send_sem, recv_sem):
    m = lax.axis_index('model')

    def store(t, v):
        if t >= 16:
            out = (dwk_out, dwv_out)[t - 16]
            out[:, 0:128] = v[0:16]
            out[:, 128:256] = v[16:32]
        else:
            h, u = divmod(t, 4)
            cols = slice((u % 2) * 128, (u % 2) * 128 + 128)
            if u < 2:
                dwo_out[h, :, cols] = v
            else:
                dwq_out[:, h, cols] = v
    ring = Ring((b0, b1, b2), (r0, r1, r2), send_sem, recv_sem, store)
    own = block(m, HALF)
    away = block(1 - m, HALF)

    def load(src, dst, i):
        return pltpu.make_async_copy(src, dst, load_sem.at[i])

    def push(src, dst, i):
        return pltpu.make_async_remote_copy(src_ref=src, dst_ref=dst, send_sem=pair_send.at[i], recv_sem=pair_recv.at[i],
                                            device_id={'model': 1 - m}, device_id_type=MESH)
    loads = [load(x_hbm, x.at[own], 0), load(wq_hbm, wq_raw, 1), load(wk_hbm, wkv.at[:, 0:E], 2), load(wv_hbm, wkv.at[:, E:2 * E], 3),
             load(dy_hbm, dy.at[own], 4), load(wo_hbm, wo, 5)]
    for i in (0, 2, 3, 1, 4, 5):
        loads[i].start()
    sem = pltpu.get_barrier_semaphore()
    ring.greet(sem)
    pl.semaphore_signal(sem, inc=1, device_id={'model': 1 - m}, device_id_type=MESH)
    dkv[...] = jnp.zeros_like(dkv)

    def project_q(h, rows):
        q[h, rows] = nn(x[rows], wq[:, block(h, E)]).astype(BF16)

    def project_do(h, rows):
        do[h, rows] = nt(dy[rows], wo[block(h, E)]).astype(BF16)

    def project_q_own(i):
        for h in range(2):
            project_q(i * 2 + h, own)

    def project_do_own(i):
        for h in range(2):
            project_do(i * 2 + h, own)

    def flatten(i):
        rows = block(i, 128)
        wq[rows] = wq_raw[rows].reshape(128, NH * E)

    def turn(i):
        cols = block(i, 256)
        kvt[0:E, cols] = kv[cols, 0:E].T
        kvt[E:2 * E, cols] = kv[cols, E:2 * E].T
    for i in (0, 2, 3):
        loads[i].wait()
    kv[own] = nn(x[own], wkv[...]).astype(BF16)
    pl.semaphore_wait(sem, 10)
    push_k = push(kv.at[own], kv.at[own], 5)
    push_x = push(x_hbm, x.at[own], 0)
    push_dy = push(dy_hbm, dy.at[own], 1)
    push_k.start()
    push_x.start()
    push_dy.start()
    loads[1].wait()
    loop(16, flatten)
    loop(2, project_q_own)
    loads[4].wait()
    loads[5].wait()
    loop(2, project_do_own)
    push_k.wait_recv()
    loop(4, turn)
    push_x.wait_recv()
    project_q(0, away)
    push_dy.wait_recv()
    project_do(0, away)

    def attend(h, j):
        n = (j + 1) * 256
        rows = slice(j * 256, n)
        qb = q[h, rows]
        dob = do[h, rows]
        st = nt(kv[0:n, 0:E], qb)
        dpt = nt(kv[0:n, E:2 * E], dob)
        yield
        keep = lax.broadcasted_iota(jnp.int32, (256, 256), 0) <= lax.broadcasted_iota(jnp.int32, (256, 256), 1)
        diag = jnp.where(keep, st[n - 256:n], -jnp.inf)
        st = diag if j == 0 else jnp.concatenate([st[0:n - 256], diag], axis=0)
        top = jnp.max(st, axis=0, keepdims=True)
        pt = jnp.exp2((st - top) * (CD * LOG2E))
        pt = pt * (1.0 / jnp.sum(pt, axis=0, keepdims=True))
        pb = pt.astype(BF16)
        yield
        ob = nn(kvt[E:2 * E, 0:n], pb).astype(BF16)
        ot[:, rows] = ob
        delta = jnp.sum(dob.T.astype(F32) * ob.astype(F32), axis=0, keepdims=True)
        dkv[0:n, E:2 * E] += nn(pb, dob)
        yield
        dst = (pt * (dpt - delta)).astype(BF16)
        yield
        dqb = (nn(kvt[0:E, 0:n], dst) * CD).astype(BF16)
        dqt[:, rows] = dqb
        dq[rows, block(h, E)] = dqb.T
        dkv[0:n, 0:E] += nn(dst, qb)
        yield

    def attention(h):
        todo = [attend(h, j) for j in (3, 2, 1, 0)]
        for tick in range(5 + 2 * 3):
            for b, stages in enumerate(todo):
                if 0 <= tick - 2 * b < 5:
                    next(stages)
            if tick == 1 and h + 1 < NH:
                project_q(h + 1, away)
            if tick == 5 and h + 1 < NH:
                project_do(h + 1, away)

    def store_tiles(t, v, i):
        sx, sy, sz = steps_of(t)
        base = (i % 2) * 2 * sy + (i // 2) * sz
        for j in range(8):
            at = base + (j % 4) * sx + (j // 4) * sy
            for u in range(2):
                b0[t + u, at] = v[j * 32:(j + 1) * 32, u * 128:(u + 1) * 128]

    def tiles_of(lhs, rhs, i):
        return nn(lhs[...], rhs[:, block(i, 512)]).astype(BF16).T

    def store_block(t, v, i):
        for u in range(2):
            store_tiles(t, v[u * 256:(u + 1) * 256], i * 2 + u)

    def grads_two(lhs, rhs, t, i):
        v = [tiles_of(lhs, rhs, i * 2 + u) for u in range(2)]
        for u in range(2):
            store_block(t, v[u], i * 2 + u)
    push_kv = push(dkv, dkv_in, 2)
    for h in range(NH - 1):
        attention(h)
        if h == 2:
            ring.finish(0, 0)

        def grads_step(i):
            vo = tiles_of(ot, dy, i)
            vq = tiles_of(dqt, x, i)
            store_block(h * 4, vo, i)
            store_block(h * 4 + 2, vq, i)
            if h > 0:
                @pl.when(i == 1)
                def _():
                    ring.middle(h - 1, 0)
        loop(4, grads_step)
        ring.start(h)
    attention(NH - 1)
    push_kv.start()
    ring.middle(0, 1)
    ring.finish(1, 0)
    loop(2, lambda i: grads_two(ot, dy, NH * 4 - 4, i))
    ring.start(3)
    loop(1, lambda i: grads_two(dqt, x, NH * 4 - 2, i))
    ring.middle(2, 0)
    loop(2, lambda i: grads_two(dqt, x, NH * 4 - 2, i), 1)
    ring.middle(1, 1)
    ring.start(4)

    def dx_away(i):
        cols = block(i, 512)
        wo[0:HALF, cols] = nt(dq[away], wq[cols]).astype(BF16)
    def push_dx(i):
        cols = pl.ds(i * 1024, 1024)
        return push(wo.at[pl.ds(0, HALF), cols], dx_in.at[:, cols], 3 + i)
    loop(1, dx_away)
    push_kv.wait_recv()

    def kv_sum(i):
        rows = block(i, 128)
        v = dkv[rows] + dkv_in[rows]
        dkvb[rows, 0:E] = (v[:, 0:E] * CD).astype(BF16)
        dkvb[rows, E:2 * E] = v[:, E:2 * E].astype(BF16)
    loop(8, kv_sum)

    def kv_block(i):
        v = tn(x[:, block(m * 4 + i, 256)], dkvb[...]).astype(BF16)
        for j in range(16):
            rows = v[j * 16:(j + 1) * 16]
            at = i * 16 + (j % 4) * 4 + j // 4
            for u in range(2):
                b0[16 + u, at, 0:16] = rows[:, u * E:u * E + 128]
                b0[16 + u, at, 16:32] = rows[:, u * E + 128:u * E + 256]
    loop(4, kv_block)
    ring.start(5)
    ring.finish(0, 1)

    loop(2, dx_away, 1)
    push_dx(0).start()
    loop(4, dx_away, 2)
    push_dx(1).start()
    for g in (3, 4, 5):
        ring.middle(g, 0)
    ring.finish(2, 0)

    def dx_own(i):
        cols = block(i, 512)
        v = nt(dq[own], wq[cols]) + nt(dkvb[own], wkv[cols])
        wo[HALF:SEQ, cols] = (v + dx_in[:, cols].astype(F32)).astype(BF16)
    push_dx(0).wait_recv()
    loop(1, dx_own)
    ring.finish(0, 2)
    loop(2, dx_own, 1)
    ring.finish(1, 1)
    push_dx(1).wait_recv()
    loop(3, dx_own, 2)
    ring.finish(4, 0)
    ring.finish(3, 0)
    loop(4, dx_own, 3)
    store_dx = load(wo.at[pl.ds(HALF, HALF)], dx_hbm, 6)
    store_dx.start()
    ring.finish(5, 0)
    ring.finish(2, 1)
    ring.finish(1, 2)
    ring.finish(4, 1)
    ring.finish(3, 1)
    ring.finish(5, 1)
    for g in (2, 4, 3):
        ring.finish(g, 2)
    stores = [load(a, b, 7 + i) for i, (a, b) in enumerate(
        ((dwq_out, dwq_hbm), (dwo_out, dwo_hbm), (dwk_out, dwk_hbm), (dwv_out, dwv_hbm)))]
    stores[0].start()
    stores[1].start()
    ring.finish(5, 2)
    stores[2].start()
    stores[3].start()
    ring.drain()
    for c in stores:
        c.wait()
    for c in (push_k, push_x, push_dy, push_kv, push_dx(0), push_dx(1)):
        c.wait_send()
    store_dx.wait()


def layer(x, dy, wq, wk, wv, wo):
    hbm = pl.BlockSpec(memory_space=pl.ANY)
    dma = pltpu.SemaphoreType.DMA
    bf = lambda *shape: pltpu.VMEM(shape, BF16)
    return pl.pallas_call(
        layer_kernel,
        out_shape=(jax.ShapeDtypeStruct((HALF, D), BF16), jax.ShapeDtypeStruct((32, NH, E), F32),
                   jax.ShapeDtypeStruct((16, E), F32), jax.ShapeDtypeStruct((16, E), F32), jax.ShapeDtypeStruct((NH, 32, E), F32)),
        in_specs=[hbm] * 6, out_specs=[hbm] * 5,
        scratch_shapes=[
            bf(SEQ, D), bf(SEQ, D), bf(D, NH, E), bf(D, NH * E), bf(D, 2 * E), bf(NH * E, D),
            bf(NH, SEQ, E), bf(NH, SEQ, E), bf(SEQ, 2 * E), bf(2 * E, SEQ), bf(E, SEQ), bf(E, SEQ), bf(SEQ, NH * E),
            pltpu.VMEM((SEQ, 2 * E), F32), pltpu.VMEM((SEQ, 2 * E), F32), bf(SEQ, 2 * E), bf(HALF, D),
            pltpu.VMEM((32, NH, E), F32), pltpu.VMEM((16, E), F32), pltpu.VMEM((16, E), F32), pltpu.VMEM((NH, 32, E), F32),
            bf(NT, 64, 32, 128), bf(NT, 16, 32, 128), bf(NT, 4, 32, 128),
            bf(NT, 3, 16, 32, 128), bf(NT, 3, 4, 32, 128), bf(NT, 3, 1, 32, 128),
            dma((11,)), dma((6,)), dma((6,)), dma((len(GROUPS),)), dma((len(GROUPS), 3, 2))],
        compiler_params=pltpu.CompilerParams(collective_id=0, has_side_effects=True, vmem_limit_bytes=67043328),
        cost_estimate=pl.CostEstimate(flops=3 * 10 ** 10, bytes_accessed=2 * 10 ** 7, transcendentals=0),
    )(x, dy, wq, wk, wv, wo)


def hand_on_kernel(dx, dwq, dwk, dwv, dwo, dx_out, dwq_out, dwk_out, dwv_out, dwo_out, dx_v, dwq_v, dwk_v, dwv_v, dwo_v, sem_in, sem_out):
    pieces = [(dx.at[pl.ds(i * 128, 128)], dx_v.at[pl.ds(i * 128, 128)], dx_out.at[pl.ds(i * 128, 128)]) for i in range(4)]
    pieces += [(dwq, dwq_v, dwq_out), (dwk, dwk_v, dwk_out), (dwv, dwv_v, dwv_out), (dwo, dwo_v, dwo_out)]
    reads = [pltpu.make_async_copy(a, b, sem_in.at[i]) for i, (a, b, _) in enumerate(pieces)]
    writes = [pltpu.make_async_copy(b, c, sem_out.at[i]) for i, (_, b, c) in enumerate(pieces)]
    for c in reads:
        c.start()
    for r, w in zip(reads, writes):
        r.wait()
        w.start()
    for w in writes:
        w.wait()


def hand_on(*arrays):
    hbm = pl.BlockSpec(memory_space=pl.ANY)
    return pl.pallas_call(
        hand_on_kernel,
        out_shape=tuple(jax.ShapeDtypeStruct(a.shape, a.dtype) for a in arrays),
        in_specs=[hbm] * 5, out_specs=[hbm] * 5,
        scratch_shapes=[pltpu.VMEM(a.shape, a.dtype) for a in arrays] + [pltpu.SemaphoreType.DMA((8,)), pltpu.SemaphoreType.DMA((8,))],
        cost_estimate=pl.CostEstimate(flops=10 ** 6, bytes_accessed=6 * 10 ** 6, transcendentals=0),
    )(*arrays)


def solution(mesh):
    tok_spec = P(('pod', 'data'), 'model', None)

    def device_step(x_loc, dy_loc, w_q, w_k, w_v, w_o):
        dx, dwq, dwk, dwv, dwo = hand_on(*layer(x_loc[0], dy_loc[0], w_q, w_k[0], w_v[0], w_o.reshape(NH * E, D)))
        return dx[None], dwq, dwk, dwv, dwo.transpose(0, 2, 1)

    kv_rows = P(('pod', 'model', 'data'), None)
    return jax.shard_map(device_step, mesh=mesh,
                         in_specs=(tok_spec, tok_spec, P(None, 'model', None), P(), P(), P('model', None, None)),
                         out_specs=(tok_spec, P(('pod', 'data'), 'model', None), kv_rows, kv_rows, P(('pod', 'model'), None, 'data')),
                         check_vma=False)
```

```python
import jax
import jax.numpy as jnp
from jax import lax
from jax.experimental import pallas as pl
from jax.experimental.pallas import tpu as pltpu
from jax.sharding import PartitionSpec as P

MESH = pl.DeviceIdType.MESH
BF16 = jnp.bfloat16
F32 = jnp.float32
NT = 18
SIZES = (16, 4, 1)
GROUPS = ((0, 4), (4, 8), (8, 12), (12, 14), (14, 16), (16, 18))
COLOURS = (0, 1, 2, 0, 1, 2, 1, 0, 2)
SEQ, HALF, D, E, NH = 1024, 512, 2048, 256, 4
CD = E ** -0.5
LOG2E = 1.4426950408889634


def nn(a, b):
    return lax.dot_general(a, b, (((1,), (0,)), ((), ())), preferred_element_type=F32)


def nt(a, b):
    return lax.dot_general(a, b, (((1,), (1,)), ((), ())), preferred_element_type=F32)


def tn(a, b):
    return lax.dot_general(a, b, (((0,), (0,)), ((), ())), preferred_element_type=F32)


def loop(n, f, start=0):
    def body(i, _):
        f(i)
        return 0
    lax.fori_loop(start, n, body, 0)


def block(i, size):
    return pl.ds(pl.multiple_of(i * size, size), size)


def steps_of(t):
    return ((16, 4, 1), (1, 16, 4), (4, 1, 16))[COLOURS[t // 2]]


class Ring:
    def __init__(self, bufs, recvs, send_sem, recv_sem, store):
        self.bufs, self.recvs, self.send_sem, self.recv_sem, self.store = bufs, recvs, send_sem, recv_sem, store
        d = lax.axis_index('data')
        coords = (d % 4, (d // 4) % 4, d // 16)
        self.at = [[((c + k) % 4, d + ((c + k) % 4 - c) * 4 ** ax) for k in range(4)] for ax, c in enumerate(coords)]

    def greet(self, sem):
        for ax in range(3):
            for k in (1, 3, 2):
                pl.semaphore_signal(sem, inc=1, device_id={'data': self.at[ax][k][1]}, device_id_type=MESH)

    def ways(self, t, p):
        ring = self.at[(COLOURS[t // 2] + p) % 3]
        return (ring[0], ring[2], ring[1], ring[3]) if t % 2 == 0 else (ring[0], ring[2], ring[3], ring[1])

    def direct(self, g, p):
        return p == 2 or (p == 1 and g >= 3)

    def msg(self, g, t, p, n):
        _, opp, fwd, back = self.ways(t, p)
        direct = self.direct(g, p)
        part = (opp, back, fwd)[n]
        to = part if direct else (fwd, back, fwd)[n]
        size = SIZES[p]
        return pltpu.make_async_remote_copy(
            src_ref=self.bufs[p].at[t, pl.ds(part[0] * size, size)], dst_ref=self.recvs[p].at[t, n],
            send_sem=self.send_sem.at[g], recv_sem=self.recv_sem.at[g, p, 0 if n == 0 and not direct else 1],
            device_id={'data': to[1]}, device_id_type=MESH)

    def arrived(self, g, p, lo, hi):
        first, last = GROUPS[g]
        ref = self.recvs[p].at[pl.ds(first, last - first), pl.ds(lo, hi - lo)]
        pltpu.make_async_copy(ref, ref, self.recv_sem.at[g, p, 0 if hi == 1 else 1]).wait()

    def tiles(self, g, f):
        for t in range(*GROUPS[g]):
            f(t)

    def start(self, g):
        for n in range(2):
            self.tiles(g, lambda t: self.msg(g, t, 0, n).start())

    def chunks(self, p, f):
        step = min(SIZES[p], 8)
        for i in range(0, SIZES[p], step):
            f(i, step)

    def middle(self, g, p):
        buf, rcv, size = self.bufs[p], self.recvs[p], SIZES[p]

        def one(t):
            fwd = self.ways(t, p)[2][0]

            def add(i, w):
                at = pl.ds(fwd * size + i, w)
                buf[t, at] = (buf[t, at].astype(F32) + rcv[t, 0, pl.ds(i, w)].astype(F32)).astype(BF16)
            self.chunks(p, add)
            self.msg(g, t, p, 2).start()
        self.arrived(g, p, 0, 1)
        self.tiles(g, one)

    def finish(self, g, p):
        buf, rcv, size = self.bufs[p], self.recvs[p], SIZES[p]
        first = 0 if self.direct(g, p) else 1

        def total(t, i, w):
            c = self.ways(t, p)[0][0]
            v = buf[t, pl.ds(c * size + i, w)].astype(F32)
            for n in range(first, 3):
                v = v + rcv[t, n, pl.ds(i, w)].astype(F32)
            return v

        def one(t):
            if p == 2:
                self.store(t, total(t, 0, 1)[0])
                return

            def put(i, w):
                self.bufs[p + 1][t, pl.ds(i, w)] = total(t, i, w).astype(BF16)
            self.chunks(p, put)
            self.msg(g, t, p + 1, 0).start()
        self.arrived(g, p, first, 3)
        self.tiles(g, one)
        if p < 2:
            for n in range(1, 3 if self.direct(g, p + 1) else 2):
                self.tiles(g, lambda t: self.msg(g, t, p + 1, n).start())

    def drain(self):
        for g, (first, last) in enumerate(GROUPS):
            ref = self.bufs[0].at[pl.ds(first, last - first), pl.ds(0, 63)]
            pltpu.make_async_copy(ref, ref, self.send_sem.at[g]).wait()


def layer_kernel(x_hbm, dy_hbm, wq_hbm, wk_hbm, wv_hbm, wo_hbm, dx_hbm, dwq_hbm, dwk_hbm, dwv_hbm, dwo_hbm,
                 x, dy, wq_raw, wq, wkv, wo, q, do, kv, kvt, ot, dqt, dq, dkv, dkv_in, dkvb, dx_in,
                 dwq_out, dwk_out, dwv_out, dwo_out, b0, b1, b2, r0, r1, r2, load_sem, pair_send, pair_recv, send_sem, recv_sem):
    m = lax.axis_index('model')

    def store(t, v):
        if t >= 16:
            out = (dwk_out, dwv_out)[t - 16]
            out[:, 0:128] = v[0:16]
            out[:, 128:256] = v[16:32]
        else:
            h, u = divmod(t, 4)
            cols = slice((u % 2) * 128, (u % 2) * 128 + 128)
            if u < 2:
                dwo_out[h, :, cols] = v
            else:
                dwq_out[:, h, cols] = v
    ring = Ring((b0, b1, b2), (r0, r1, r2), send_sem, recv_sem, store)
    own = block(m, HALF)
    away = block(1 - m, HALF)

    def load(src, dst, i):
        return pltpu.make_async_copy(src, dst, load_sem.at[i])

    def push(src, dst, i):
        return pltpu.make_async_remote_copy(src_ref=src, dst_ref=dst, send_sem=pair_send.at[i], recv_sem=pair_recv.at[i],
                                            device_id={'model': 1 - m}, device_id_type=MESH)
    loads = [load(x_hbm, x.at[own], 0), load(wq_hbm, wq_raw, 1), load(wk_hbm, wkv.at[:, 0:E], 2), load(wv_hbm, wkv.at[:, E:2 * E], 3),
             load(dy_hbm, dy.at[own], 4), load(wo_hbm, wo, 5)]
    for i in (0, 2, 3, 1, 4, 5):
        loads[i].start()
    sem = pltpu.get_barrier_semaphore()
    ring.greet(sem)
    pl.semaphore_signal(sem, inc=1, device_id={'model': 1 - m}, device_id_type=MESH)
    dkv[...] = jnp.zeros_like(dkv)

    def project_q(h, rows):
        q[h, rows] = nn(x[rows], wq[:, block(h, E)]).astype(BF16)

    def project_do(h, rows):
        do[h, rows] = nt(dy[rows], wo[block(h, E)]).astype(BF16)

    def project_q_own(i):
        for h in range(2):
            project_q(i * 2 + h, own)

    def project_do_own(i):
        for h in range(2):
            project_do(i * 2 + h, own)

    def flatten(i):
        rows = block(i, 128)
        wq[rows] = wq_raw[rows].reshape(128, NH * E)

    def turn(i):
        cols = block(i, 256)
        kvt[0:E, cols] = kv[cols, 0:E].T
        kvt[E:2 * E, cols] = kv[cols, E:2 * E].T
    for i in (0, 2, 3):
        loads[i].wait()
    kv[own] = nn(x[own], wkv[...]).astype(BF16)
    pl.semaphore_wait(sem, 10)
    push_k = push(kv.at[own], kv.at[own], 5)
    push_x = push(x_hbm, x.at[own], 0)
    push_dy = push(dy_hbm, dy.at[own], 1)
    push_k.start()
    push_x.start()
    push_dy.start()
    loads[1].wait()
    loop(16, flatten)
    loop(2, project_q_own)
    loads[4].wait()
    loads[5].wait()
    loop(2, project_do_own)
    push_k.wait_recv()
    loop(4, turn)
    push_x.wait_recv()
    project_q(0, away)
    push_dy.wait_recv()
    project_do(0, away)

    def attend(h, j):
        n = (j + 1) * 256
        rows = slice(j * 256, n)
        qb = q[h, rows]
        dob = do[h, rows]
        st = nt(kv[0:n, 0:E], qb)
        dpt = nt(kv[0:n, E:2 * E], dob)
        yield
        keep = lax.broadcasted_iota(jnp.int32, (256, 256), 0) <= lax.broadcasted_iota(jnp.int32, (256, 256), 1)
        diag = jnp.where(keep, st[n - 256:n], -jnp.inf)
        st = diag if j == 0 else jnp.concatenate([st[0:n - 256], diag], axis=0)
        top = jnp.max(st, axis=0, keepdims=True)
        pt = jnp.exp2((st - top) * (CD * LOG2E))
        pt = pt * (1.0 / jnp.sum(pt, axis=0, keepdims=True))
        pb = pt.astype(BF16)
        yield
        ob = nn(kvt[E:2 * E, 0:n], pb).astype(BF16)
        ot[:, rows] = ob
        delta = jnp.sum(dob.T.astype(F32) * ob.astype(F32), axis=0, keepdims=True)
        dkv[0:n, E:2 * E] += nn(pb, dob)
        yield
        dst = (pt * (dpt - delta)).astype(BF16)
        yield
        dqb = (nn(kvt[0:E, 0:n], dst) * CD).astype(BF16)
        dqt[:, rows] = dqb
        dq[rows, block(h, E)] = dqb.T
        dkv[0:n, 0:E] += nn(dst, qb)
        yield

    def attention(h):
        todo = [attend(h, j) for j in (3, 2, 1, 0)]
        for tick in range(5 + 2 * 3):
            for b, stages in enumerate(todo):
                if 0 <= tick - 2 * b < 5:
                    next(stages)
            if tick == 1 and h + 1 < NH:
                project_q(h + 1, away)
            if tick == 5 and h + 1 < NH:
                project_do(h + 1, away)

    def store_tiles(t, v, i):
        sx, sy, sz = steps_of(t)
        base = (i % 2) * 2 * sy + (i // 2) * sz
        for j in range(8):
            at = base + (j % 4) * sx + (j // 4) * sy
            for u in range(2):
                b0[t + u, at] = v[j * 32:(j + 1) * 32, u * 128:(u + 1) * 128]

    def tiles_of(lhs, rhs, i):
        return nn(lhs[...], rhs[:, block(i, 512)]).astype(BF16).T

    def store_block(t, v, i):
        for u in range(2):
            store_tiles(t, v[u * 256:(u + 1) * 256], i * 2 + u)

    def grads_two(lhs, rhs, t, i):
        v = [tiles_of(lhs, rhs, i * 2 + u) for u in range(2)]
        for u in range(2):
            store_block(t, v[u], i * 2 + u)
    push_kv = push(dkv, dkv_in, 2)
    for h in range(NH - 1):
        attention(h)
        if h == 2:
            ring.finish(0, 0)

        def grads_step(i):
            vo = tiles_of(ot, dy, i)
            vq = tiles_of(dqt, x, i)
            store_block(h * 4, vo, i)
            store_block(h * 4 + 2, vq, i)
            if h > 0:
                @pl.when(i == 1)
                def _():
                    ring.middle(h - 1, 0)
        loop(4, grads_step)
        ring.start(h)
    attention(NH - 1)
    push_kv.start()
    ring.middle(0, 1)
    ring.finish(1, 0)
    loop(2, lambda i: grads_two(ot, dy, NH * 4 - 4, i))
    ring.start(3)
    loop(1, lambda i: grads_two(dqt, x, NH * 4 - 2, i))
    ring.middle(2, 0)
    loop(2, lambda i: grads_two(dqt, x, NH * 4 - 2, i), 1)
    ring.middle(1, 1)
    ring.start(4)

    def dx_away(i):
        cols = block(i, 512)
        wo[0:HALF, cols] = nt(dq[away], wq[cols]).astype(BF16)
    def push_dx(i):
        cols = pl.ds(i * 1024, 1024)
        return push(wo.at[pl.ds(0, HALF), cols], dx_in.at[:, cols], 3 + i)
    push_kv.wait_recv()

    def kv_sum(i):
        rows = block(i, 128)
        v = dkv[rows] + dkv_in[rows]
        dkvb[rows, 0:E] = (v[:, 0:E] * CD).astype(BF16)
        dkvb[rows, E:2 * E] = v[:, E:2 * E].astype(BF16)
    loop(8, kv_sum)

    def kv_block(i):
        v = tn(x[:, block(m * 4 + i, 256)], dkvb[...]).astype(BF16)
        for j in range(16):
            rows = v[j * 16:(j + 1) * 16]
            at = i * 16 + (j % 4) * 4 + j // 4
            for u in range(2):
                b0[16 + u, at, 0:16] = rows[:, u * E:u * E + 128]
                b0[16 + u, at, 16:32] = rows[:, u * E + 128:u * E + 256]
    loop(4, kv_block)
    ring.start(5)
    ring.finish(0, 1)

    loop(2, dx_away)
    push_dx(0).start()
    loop(4, dx_away, 2)
    push_dx(1).start()
    ring.middle(3, 0)
    ring.middle(4, 0)
    ring.middle(5, 0)

    def dx_own(i):
        cols = block(i, 512)
        v = nt(dq[own], wq[cols]) + nt(dkvb[own], wkv[cols])
        wo[HALF:SEQ, cols] = (v + dx_in[:, cols].astype(F32)).astype(BF16)
    push_dx(0).wait_recv()
    loop(2, dx_own)
    ring.finish(2, 0)
    push_dx(1).wait_recv()
    loop(3, dx_own, 2)
    ring.finish(0, 2)
    ring.finish(1, 1)
    loop(4, dx_own, 3)
    store_dx = load(wo.at[pl.ds(HALF, HALF)], dx_hbm, 6)
    store_dx.start()
    ring.finish(4, 0)
    ring.finish(3, 0)
    ring.finish(5, 0)
    ring.middle(2, 1)
    ring.finish(1, 2)
    ring.finish(4, 1)
    ring.finish(3, 1)
    ring.finish(5, 1)
    ring.finish(2, 1)
    for g in (4, 3, 2):
        ring.finish(g, 2)
    stores = [load(a, b, 7 + i) for i, (a, b) in enumerate(
        ((dwq_out, dwq_hbm), (dwo_out, dwo_hbm), (dwk_out, dwk_hbm), (dwv_out, dwv_hbm)))]
    stores[0].start()
    stores[1].start()
    ring.finish(5, 2)
    stores[2].start()
    stores[3].start()
    ring.drain()
    for c in stores:
        c.wait()
    for c in (push_k, push_x, push_dy, push_kv, push_dx(0), push_dx(1)):
        c.wait_send()
    store_dx.wait()


def layer(x, dy, wq, wk, wv, wo):
    hbm = pl.BlockSpec(memory_space=pl.ANY)
    dma = pltpu.SemaphoreType.DMA
    bf = lambda *shape: pltpu.VMEM(shape, BF16)
    return pl.pallas_call(
        layer_kernel,
        out_shape=(jax.ShapeDtypeStruct((HALF, D), BF16), jax.ShapeDtypeStruct((32, NH, E), F32),
                   jax.ShapeDtypeStruct((16, E), F32), jax.ShapeDtypeStruct((16, E), F32), jax.ShapeDtypeStruct((NH, 32, E), F32)),
        in_specs=[hbm] * 6, out_specs=[hbm] * 5,
        scratch_shapes=[
            bf(SEQ, D), bf(SEQ, D), bf(D, NH, E), bf(D, NH * E), bf(D, 2 * E), bf(NH * E, D),
            bf(NH, SEQ, E), bf(NH, SEQ, E), bf(SEQ, 2 * E), bf(2 * E, SEQ), bf(E, SEQ), bf(E, SEQ), bf(SEQ, NH * E),
            pltpu.VMEM((SEQ, 2 * E), F32), pltpu.VMEM((SEQ, 2 * E), F32), bf(SEQ, 2 * E), bf(HALF, D),
            pltpu.VMEM((32, NH, E), F32), pltpu.VMEM((16, E), F32), pltpu.VMEM((16, E), F32), pltpu.VMEM((NH, 32, E), F32),
            bf(NT, 64, 32, 128), bf(NT, 16, 32, 128), bf(NT, 4, 32, 128),
            bf(NT, 3, 16, 32, 128), bf(NT, 3, 4, 32, 128), bf(NT, 3, 1, 32, 128),
            dma((11,)), dma((6,)), dma((6,)), dma((len(GROUPS),)), dma((len(GROUPS), 3, 2))],
        compiler_params=pltpu.CompilerParams(collective_id=0, has_side_effects=True, vmem_limit_bytes=67043328),
        cost_estimate=pl.CostEstimate(flops=3 * 10 ** 10, bytes_accessed=2 * 10 ** 7, transcendentals=0),
    )(x, dy, wq, wk, wv, wo)


def hand_on_kernel(dx, dwq, dwk, dwv, dwo, dx_out, dwq_out, dwk_out, dwv_out, dwo_out, dx_v, dwq_v, dwk_v, dwv_v, dwo_v, sem_in, sem_out):
    pieces = [(dx.at[pl.ds(i * 128, 128)], dx_v.at[pl.ds(i * 128, 128)], dx_out.at[pl.ds(i * 128, 128)]) for i in range(4)]
    pieces += [(dwq, dwq_v, dwq_out), (dwk, dwk_v, dwk_out), (dwv, dwv_v, dwv_out), (dwo, dwo_v, dwo_out)]
    reads = [pltpu.make_async_copy(a, b, sem_in.at[i]) for i, (a, b, _) in enumerate(pieces)]
    writes = [pltpu.make_async_copy(b, c, sem_out.at[i]) for i, (_, b, c) in enumerate(pieces)]
    for c in reads:
        c.start()
    for r, w in zip(reads, writes):
        r.wait()
        w.start()
    for w in writes:
        w.wait()


def hand_on(*arrays):
    hbm = pl.BlockSpec(memory_space=pl.ANY)
    return pl.pallas_call(
        hand_on_kernel,
        out_shape=tuple(jax.ShapeDtypeStruct(a.shape, a.dtype) for a in arrays),
        in_specs=[hbm] * 5, out_specs=[hbm] * 5,
        scratch_shapes=[pltpu.VMEM(a.shape, a.dtype) for a in arrays] + [pltpu.SemaphoreType.DMA((8,)), pltpu.SemaphoreType.DMA((8,))],
        cost_estimate=pl.CostEstimate(flops=10 ** 6, bytes_accessed=6 * 10 ** 6, transcendentals=0),
    )(*arrays)


def solution(mesh):
    tok_spec = P(('pod', 'data'), 'model', None)

    def device_step(x_loc, dy_loc, w_q, w_k, w_v, w_o):
        dx, dwq, dwk, dwv, dwo = hand_on(*layer(x_loc[0], dy_loc[0], w_q, w_k[0], w_v[0], w_o.reshape(NH * E, D)))
        return dx[None], dwq, dwk, dwv, dwo.transpose(0, 2, 1)

    kv_rows = P(('pod', 'model', 'data'), None)
    return jax.shard_map(device_step, mesh=mesh,
                         in_specs=(tok_spec, tok_spec, P(None, 'model', None), P(), P(), P('model', None, None)),
                         out_specs=(tok_spec, P(('pod', 'data'), 'model', None), kv_rows, kv_rows, P(('pod', 'model'), None, 'data')),
                         check_vma=False)
```
